32 devices in a mesh: rep: 1, dp: 32 (over x, y, z, core).
Axes of the slice: x: 2, y: 2, z: 4, core: 2. Of those that a mesh axis runs over, the one named last changes fastest.
Arguments:
- g_w_gate: bfloat16 [32, 2, 1152, 4608], P(('rep', 'dp'))
- g_w_up: bfloat16 [32, 2, 1152, 4608], P(('rep', 'dp'))
- g_w_down: bfloat16 [32, 2, 4608, 1152], P(('rep', 'dp'))
- w_gate: bfloat16 [2, 1152, 4608], replicated
- w_up: bfloat16 [2, 1152, 4608], replicated
- w_down: bfloat16 [2, 4608, 1152], replicated
- m_w_gate: float32 [2, 1152, 4608], P(None, 'dp')
- m_w_up: float32 [2, 1152, 4608], P(None, 'dp')
- m_w_down: float32 [2, 4608, 1152], P(None, 'dp')
- v_w_gate: float32 [2, 1152, 4608], P(None, 'dp')
- v_w_up: float32 [2, 1152, 4608], P(None, 'dp')
- v_w_down: float32 [2, 4608, 1152], P(None, 'dp')
Outputs:
- output 1: bfloat16 [2, 1152, 4608], P('rep')
- output 2: bfloat16 [2, 1152, 4608], P('rep')
- output 3: bfloat16 [2, 4608, 1152], P('rep')
- output 4: float32 [2, 1152, 4608], P('rep', 'dp')
- output 5: float32 [2, 1152, 4608], P('rep', 'dp')
- output 6: float32 [2, 4608, 1152], P('rep', 'dp')
- output 7: float32 [2, 1152, 4608], P('rep', 'dp')
- output 8: float32 [2, 1152, 4608], P('rep', 'dp')
- output 9: float32 [2, 4608, 1152], P('rep', 'dp')
All inputs are finite; a program needn't handle non-finite values.
Results may differ from the reference program's by a relative error of at most 0.022.
Values are sent between devices in bfloat16 or wider.
A program may use at most 2 GiB of HBM per device.

```python
import jax
import jax.numpy as jnp
from jax import lax

DEVICES = 32
D = 1152
FF = 4608
LAYERS = 2
NAMES = ("w_gate", "w_up", "w_down")
SHAPES = {"w_gate": (LAYERS, D, FF), "w_up": (LAYERS, D, FF), "w_down": (LAYERS, FF, D)}


def setup_inputs(seed: int = 0, part: int = 0) -> dict:
    kz, *keys = jax.random.split(jax.random.key(seed), 1 + 5 * len(NAMES))
    loud = 2.0 ** jax.random.uniform(kz, (), jnp.float32, -1.0, 1.0)
    drawn = {}
    for name, key, both in zip(NAMES, keys[:3], keys[3:6], strict=True):
        own = jax.random.normal(jax.random.fold_in(key, part), (DEVICES, *SHAPES[name]), jnp.float32)
        shared = jax.random.normal(jax.random.fold_in(both, part), SHAPES[name], jnp.float32)
        drawn["g_" + name] = (loud * (0.7 * shared / DEVICES + 0.7 * own * DEVICES**-0.5)).astype(jnp.bfloat16)
    for name, key in zip(NAMES, keys[6:9], strict=True):
        drawn[name] = (jax.random.normal(key, SHAPES[name], jnp.float32) * SHAPES[name][1] ** -0.5).astype(jnp.bfloat16)
    for name, key in zip(NAMES, keys[9:12], strict=True):
        drawn["m_" + name] = loud * 0.5 * jax.random.normal(key, SHAPES[name], jnp.float32)
    for name, key in zip(NAMES, keys[12:15], strict=True):
        drawn["v_" + name] = loud * loud * jax.random.uniform(key, SHAPES[name], jnp.float32, 0.5, 1.5)
    return drawn


def adamw(w, m, v, g):
    m = 0.9 * m + 0.1 * g
    v = 0.95 * v + 0.05 * g * g
    step = m * lax.rsqrt(v + 1e-8) + 0.1 * w
    return (w - 0.02 * step).astype(jnp.bfloat16), m, v


def clipped(gradients, sum_of_squares, count):
    factor = jnp.minimum(1.0, 0.5 * lax.rsqrt(sum_of_squares / count + 1e-30))
    return [g * factor for g in gradients]


def reference(g_w_gate, g_w_up, g_w_down, w_gate, w_up, w_down, m_w_gate, m_w_up, m_w_down, v_w_gate, v_w_up, v_w_down):
    def total(terms):
        return lax.scan(lambda so_far, term: (so_far + term.astype(jnp.float32), None), jnp.zeros(terms.shape[1:], jnp.float32), terms)[0]

    gradients = [total(terms).astype(jnp.bfloat16).astype(jnp.float32) for terms in (g_w_gate, g_w_up, g_w_down)]
    gradients = clipped(gradients, sum(jnp.sum(g * g) for g in gradients), sum(g.size for g in gradients))
    new = [
        adamw(w.astype(jnp.float32), m, v, g)
        for w, m, v, g in zip((w_gate, w_up, w_down), (m_w_gate, m_w_up, m_w_down), (v_w_gate, v_w_up, v_w_down), gradients, strict=True)
    ]
    return tuple(one[which] for which in range(3) for one in new)
```

```python
import functools

import jax
import jax.numpy as jnp
from jax import lax
from jax.experimental import pallas as pl
from jax.experimental.pallas import tpu as pltpu
from jax.sharding import PartitionSpec as P

MESH = pl.DeviceIdType.MESH
BF, F32 = jnp.bfloat16, jnp.float32
DMA = pltpu.SemaphoreType.DMA
VMEM, HBM = pltpu.VMEM, pltpu.HBM
ALL = slice(None)
L, X, Y, Z, U, CORES = 2, 2, 2, 4, 9, 2
N = X * Y * Z * CORES
SUB, ROWS, LANES = 8, 16, 128
T3 = (U, ROWS, LANES)
NP = 3 * L
HALF = NP - L
OWN = 5
PART = {'A': pl.ds(0, OWN), 'B': pl.ds(OWN, 3), 'C': U - 1}
VM, HB, ANY = (pl.BlockSpec(memory_space=s) for s in (VMEM, HBM, pl.ANY))


def tiled(a):
    l, r, c = a.shape
    return a.reshape(l, r // SUB, SUB, c // LANES, LANES).swapaxes(2, 3)


def untiled(a, r, c):
    return a.reshape(L, r // SUB, c // LANES, SUB, LANES).swapaxes(2, 3).reshape(L, r, c)


def view_gu(g): return tiled(g).reshape(L, X, Y, Z, U, CORES, *T3)
def view_d(g): return tiled(g).reshape(L, X, Y, Z, CORES, U, *T3)


def place():
    d = lax.axis_index("dp")
    d, c = d // CORES, d % CORES
    d, z = d // Z, d % Z
    return d // Y, d % Y, z, c


def dev(x, y, z, c): return 0, ((x * Y + y) * Z + z) * CORES + c


def line(z):
    h = z // 2
    return (z == 1) | (z == 2), [z, 1 - z + Z * h, 2 - h, 3 - 3 * h], z + 1 - 2 * h, 3 * h


def over(n, f): lax.fori_loop(0, n, lambda i, _: (f(i), 0)[1], 0)


def copy(src, dst, sem): return pltpu.make_async_copy(src, dst, sem)


def remote(src, dst, ss, rs, to): return pltpu.make_async_remote_copy(src, dst, ss, rs, device_id=to, device_id_type=MESH)


def got(ref, sem): copy(ref, ref, sem).wait()


def split(name): return name[0], name[1], int(name[-1]) if name[-1].isdigit() else 0


def lagged(names): return [(n.rstrip('+'), n.count('+')) for n in names]


RS_ORDER = ['By0', 'Ax0', 'Ax7+', 'Cz0', 'By2', 'Bf++', 'Az1+', 'Ax1', 'Ax4', 'Cz1', 'By1', 'Ax2', 'Cz2', 'Ax6', 'Ax5', 'Bx+', 'Ay0', 'Bz0', 'Ay1', 'Bz2', 'Ax3', 'By3', 'Bz1', 'Ay2', 'Az0', 'Cx', 'Ay3+', 'Az2+', 'Af++', 'Cf++', 'Cy+']
TURN = 24
CLASSES = {
    'A': ((OWN,), ['Ax0', 'Ax1', 'Ax2', 'Ax3', 'Ax4', 'Ax5', 'Ax6', 'Ax7', 'Ay0', 'Ay1', 'Ay2', 'Ay3', 'Az0', 'Az1', 'Az2', 'Af']),
    'By': ((X, 3), ['By0', 'By1', 'By2', 'By3', 'Bz0', 'Bz1', 'Bz2']),
    'Bx': ((3,), ['Bx', 'Bf']),
    'Cz': ((X, Y), ['Cz0', 'Cz1', 'Cz2']),
    'Cx': ((Y,), ['Cx']),
    'Cy': ((), ['Cy', 'Cf']),
}
CLASS_OF = {n: (k, i) for k, (_, names) in CLASSES.items() for i, n in enumerate(names)}
ARRIVE = {'Ax': (8, 'A'), 'Ay': (Z, 'A'), 'Az': (5, 'A'), 'By': (Z, 'By'), 'Bz': (5, 'By'), 'Bx': (1, 'Bx'), 'Cz': (5, 'Cz'), 'Cx': (1, 'Cx'), 'Cy': (1, 'Cy')}
LAST, CROSS = 2, 4


def rs_kernel(order, gg, gu, gd, Ggu, Gd, TOT, PARTNER, *scr):
    scr = iter(scr)
    take = lambda names: {n: next(scr) for n in names}
    own, par, snd, rcv = take(CLASSES), take(CLASSES), take(CLASSES), take(ARRIVE)
    fin, gx, acc, sall = take(range(4)).values()
    own_s, par_s, snd_s, first_s, rcv_s = take(CLASSES), take(CLASSES), take(CLASSES), take(CLASSES), take(ARRIVE)
    d2d_ss, d2d_rs, gx_ss, gx_rs, sa_ss, sa_rs = take(range(6)).values()
    x, y, z, c = place()
    ox, oy, oc = 1 - x, 1 - y, 1 - c
    me = lax.axis_index("dp")
    mid, near, inner, _ = line(z)
    zo = near[::-1]
    side = z + 1 - 2 * (z % 2)
    NX, NY, NC = dev(ox, y, z, c), dev(x, oy, z, c), dev(x, y, z, oc)

    def block(name):
        n, axis, i = split(name)
        u = PART[n]
        if axis == 'f': return x, y, z, u
        if n == 'A':
            if axis == 'x': return ox, (oy if i < Z else y), zo[i % Z], u
            return x, (oy if axis == 'y' else y), zo[i], u
        if n == 'B':
            if axis == 'x': return ox, y, z, u
            return ALL, (oy if axis == 'y' else y), zo[i], u
        return {'z': (ALL, ALL, zo[i], u), 'x': (ox, ALL, z, u), 'y': (x, oy, z, u)}[axis]

    def cut(k, l, b, core):
        return gd.at[(l, *b[:3], core, b[3])] if k == 2 else (gg, gu)[k].at[(l, *b, core)]

    def reload(name, p):
        cl, i = CLASS_OF[name]
        b = block(name)
        @pl.when((p >= 0) & (p < NP))
        def _():
            for k in range(3):
                @pl.when(p // L == k)
                def _(): copy(cut(k, p % L, b, c), own[cl].at[i], own_s[cl].at[i]).start()
            @pl.when(p > 0)
            def _(): copy(PARTNER.at[(p, *b)], par[cl].at[i], par_s[cl].at[i]).start()

    def send(name, p):
        cl, i = CLASS_OF[name]
        n, axis, j = split(name)
        if axis == 'x': to, slot = NX, j
        elif axis == 'y': to, slot = NY, j
        elif j < 2: to, slot = dev(x, y, inner, c), j + 3 * mid.astype(jnp.int32)
        else: to, slot = dev(x, y, side, c), LAST
        kind = name[:2]
        return remote(snd[cl].at[i], rcv[kind].at[p, slot], snd_s[cl].at[i], rcv_s[kind].at[p, slot], to)

    def add(dst, refs, lead, last):
        def one(*idx):
            at = idx if idx else ...
            t = sum(r[at].astype(F32) for r in refs).astype(BF)
            dst[at] = t
            if last:
                t = t.astype(F32)
                acc[...] += jnp.sum(t * t, axis=0)
        if not lead: one()
        elif len(lead) == 1: over(lead[0], one)
        else: over(lead[0], lambda i: over(lead[1], lambda j: one(i, j)))

    def task(name, p):
        cl, i = CLASS_OF[name]
        n, axis, j = split(name)
        lead = CLASSES[cl][0]
        R = lambda kind, s: rcv[kind].at[p, s]
        def arrive(*which):
            for kind, s in which: got(R(kind, s), rcv_s[kind].at[p, s])
        got(own[cl].at[i], own_s[cl].at[i])
        got(par[cl].at[i], par_s[cl].at[i])
        zk, refs, far, wait, farwait = n + 'z', [], [], [], []
        if axis == 'z':
            s = (0, 1, 3)[j]
            far, farwait = [R(zk, s)], [(zk, s)]
            wait = {'A': [('Ax', Z + j), ('Ay', j)], 'B': [('By', j)], 'C': []}[n]
            refs = [R(*w) for w in wait]
        elif name[:2] == 'Ay':
            wait = [('Ax', j)]
            refs = [R(*w) for w in wait]
        elif name == 'Af':
            wait, farwait = [('Ax', Z + 3), ('Ay', 3), (zk, LAST)], [(zk, CROSS)]
            refs, far = [R(*w) for w in wait], [R(zk, CROSS)]
        elif axis != 'y' or n == 'C':
            if n == 'B' and axis == 'x' or n == 'C' and axis == 'x': wait, farwait = [(zk, LAST)], [(zk, CROSS)]
            if name == 'Bx': wait += [('By', 3)]
            if name in ('Bf', 'Cy'): wait = [(n + 'x', 0)]
            if name == 'Cf': wait = [('Cy', 0)]
            here = {'Bx': (ox,), 'Bf': (x,), 'Cx': (ox,), 'Cy': (x, oy), 'Cf': (x, y)}.get(name)
            if here:
                refs, far = [R(zk, LAST).at[here]], [R(zk, CROSS).at[here]]
                if n == 'B': refs += [R('By', 3).at[here]]
                if name == 'Bf': refs += [R('Bx', 0)]
                if name == 'Cy': refs += [R('Cx', 0).at[oy]]
                if name == 'Cf': refs += [R('Cx', 0).at[y], R('Cy', 0)]
        arrive(*wait)
        last = axis == 'f'
        if last: dst = fin.at[p, PART[n]]
        else:
            @pl.when(p > 0)
            def _(): send(name, p).wait_send()
            dst = snd[cl].at[i]
        refs = [own[cl].at[i], par[cl].at[i]] + refs
        if far:
            @pl.when(mid)
            def _():
                arrive(*farwait)
                add(dst, refs + far, lead, last)
            @pl.when(jnp.logical_not(mid))
            def _(): add(dst, refs, lead, last)
        else: add(dst, refs, lead, last)
        if not last: send(name, p).start()

    def swap0(name):
        cl, i = CLASS_OF[name]
        return remote(cut(0, 0, block(name), oc), par[cl].at[i], first_s[cl].at[i], par_s[cl].at[i], NC)

    def swap(p):
        parts = [(ox, ALL, ALL, PART['A']), (ALL, ALL, ALL, PART['B']), (ALL, ALL, ALL, PART['C']), (x, ALL, ALL, PART['A'])]
        return [remote(cut(p // L, p % L, q, oc), PARTNER.at[(p, *q)], d2d_ss.at[p, i], d2d_rs.at[p, i], NC) for i, q in enumerate(parts)]

    acc[...] = jnp.zeros_like(acc)
    for n, _ in order: reload(n, jnp.int32(0))
    b = pltpu.get_barrier_semaphore()
    def others(f):
        def one(i):
            @pl.when(i != me)
            def _(): f((0, i))
        over(N, one)
    others(lambda to: pl.semaphore_signal(b, 1, device_id=to, device_id_type=MESH))
    pl.semaphore_wait(b, N - 1)
    for n, _ in sorted(order, key=lambda t: t[1]): swap0(n).start()
    for p in range(1, NP):
        for cp in swap(p): cp.start()

    finlag = max(lag for n, lag in order if n[1] == 'f')
    def rows(p): return remote(fin.at[p, pl.ds(Z * oc, OWN)], gx.at[p], gx_ss.at[p], gx_rs.at[p], NC)
    def round_(r):
        for i, (n, lag) in enumerate(order):
            p = r - lag
            @pl.when((p >= 0) & (p < NP))
            def _(): task(n, p)
            if i == TURN:
                for q in range(1, NP):
                    @pl.when(q == r + 1)
                    def _():
                        for cp in swap(q): cp.wait_recv()
                for m, ml in order[:TURN]:
                    @pl.when(r >= ml)
                    def _(): reload(m, r - ml + 1)
            if i >= TURN:
                @pl.when(p >= 0)
                def _(): reload(n, p + 1)
        q = r - finlag
        @pl.when((q >= 0) & (q < HALF))
        def _(): rows(q).start()
    over(NP + max(lag for _, lag in order), round_)

    sall[me] = acc[0:SUB] + acc[SUB:ROWS]
    others(lambda to: remote(sall.at[me], sall.at[me], sa_ss, sa_rs, to).start())
    for l in range(L): Gd[l] = fin[HALF + l]
    for p in range(HALF):
        k, l = p // L, p % L
        Ggu[k, l, :, c] = fin[p, pl.ds(Z * c, OWN)]
        rows(p).wait()
        Ggu[k, l, :, oc] = gx[p]
    for n, lag in order:
        swap0(n).wait_send()
        if n[1] != 'f': send(n, NP - 1).wait_send()
    for p in range(1, NP):
        for cp in swap(p): cp.wait_send()
    rest = sall.at[pl.ds(0, N - 1)]
    got(rest, sa_rs)
    got(rest, sa_ss)
    TOT[...] = jnp.sum(sall[...], axis=0)


def rs_call(gg, gu, gd):
    bufs = [VMEM((len(names), *shape, *T3), BF) for shape, names in CLASSES.values()]
    sems = [DMA((len(names),)) for _, names in CLASSES.values()]
    scratch = bufs * 3 + [VMEM((NP, n, *CLASSES[cl][0], *T3), BF) for n, cl in ARRIVE.values()]
    scratch += [VMEM((NP, U, *T3), BF), VMEM((HALF, OWN, *T3), BF), VMEM((ROWS, LANES), F32), VMEM((N, SUB, LANES), F32)]
    scratch += sems * 4 + [DMA((NP, n)) for n, _ in ARRIVE.values()]
    scratch += [DMA((NP, 4)), DMA((NP, 4)), DMA((HALF,)), DMA((HALF,)), DMA(()), DMA(())]
    return pl.pallas_call(
        functools.partial(rs_kernel, lagged(RS_ORDER)),
        out_shape=(VMEM((2, L, OWN, CORES, *T3), BF), VMEM((L, U, *T3), BF), VMEM((SUB, LANES), F32), HBM((NP, X, Y, Z, U, *T3), BF)),
        in_specs=[ANY] * 3,
        out_specs=(VM, VM, VM, HB),
        scratch_shapes=scratch,
        compiler_params=pltpu.CompilerParams(collective_id=0, has_side_effects=True, vmem_limit_bytes=58 * 2**20),
        name="reduce_scatter",
    )(view_gu(gg), view_gu(gu), view_d(gd))


BLOCK, TILES = 36, 36
RUN = TILES * L


def up_kernel(count, Ggu, Gd, TOT, wg, wu, wd, *refs):
    moments, (Wgu, Wd), new, scr = refs[:6], refs[6:8], refs[8:14], refs[14:]
    mom, dm, dv, wb, wdb, ld, st = scr
    x, y, z, c = place()
    loads, stores = [], []
    def start(kept, sems, src, dst):
        kept.append(copy(src, dst, sems.at[len(kept)]))
        kept[-1].start()
    load, store = functools.partial(start, loads, ld), functools.partial(start, stores, st)
    rows = pl.ds(Z, BLOCK)
    load(moments[2], dm)
    load(moments[5], dv)
    load(wd.at[:, x, y, z, c], wdb)
    for k in range(2):
        for i in range(2): load(moments[k + 3 * i], mom.at[k, i, rows])
        load((wg, wu)[k].at[:, x, y, z, pl.ds(Z * c, OWN)], wb.at[k])
    for k in range(2):
        for i in range(2):
            for at in (0, Z + BLOCK): mom[k, i, at:at + Z] = jnp.zeros((Z, TILES, L, LANES), F32)
    s = jnp.sum(jnp.sum(TOT[...], axis=0, keepdims=True), axis=1, keepdims=True)
    factor = jnp.minimum(1.0, 0.5 * lax.rsqrt(s * (1.0 / count) + 1e-30))
    def adamw(w, m, v, g):
        g = g * factor
        m = 0.9 * m + 0.1 * g
        v = 0.95 * v + 0.05 * g * g
        return w - 0.02 * (m * lax.rsqrt(v + 1e-8) + 0.1 * w), m, v
    for cp in loads[:3]: cp.wait()
    def down(l):
        def unit(u):
            for j in range(U):
                at = (l, u, j)
                w, dm[at], dv[at] = adamw(wdb[at].astype(F32), dm[at], dv[at], Gd[at].astype(F32))
                wdb[at] = w.astype(BF)
        over(U, unit)
    over(L, down)
    store(wdb, Wd)
    store(dm, new[2])
    store(dv, new[5])
    for k in range(2):
        for cp in loads[3 + 3 * k:][:3]: cp.wait()
        M, V = (mom.at[k, i].reshape((BLOCK + 2 * Z) * RUN, LANES) for i in range(2))
        def tile(l, u, ch):
            base = (SUB * u + Z - Z * c) * RUN + TILES * ch + l
            for j in range(U):
                g, w = Ggu[k, l, u, ch, j].astype(F32), wb[k, l, u, ch, j].astype(F32)
                half = []
                for e in range(2):
                    at = pl.ds(base + (2 * j + e) * L, SUB, stride=RUN)
                    h = slice(SUB * e, SUB * e + SUB)
                    wn, M[at, :], V[at, :] = adamw(w[h], M[at, :], V[at, :], g[h])
                    half.append(wn)
                wb[k, l, u, ch, j] = jnp.concatenate(half).astype(BF)
        over(L, lambda l: over(OWN, lambda u: over(CORES, lambda ch: tile(l, u, ch))))
        store(wb.at[k], Wgu.at[pl.ds(L * k, L)])
        for i in range(2): store(mom.at[k, i, rows], new[k + 3 * i])
    for cp in stores: cp.wait()


def view_m(m): return m.reshape(L, BLOCK, TILES, LANES).transpose(1, 2, 0, 3)
def unview_m(m): return m.transpose(2, 0, 1, 3).reshape(L, BLOCK, TILES * LANES)
def view_md(m): return tiled(m).reshape(L, U, *T3)


def up_call(Ggu, Gd, total, weights, m, v):
    moments = [f(a) for a, f in zip((*m, *v), (view_m, view_m, view_md) * 2)]
    count = sum(w.size for w in weights)
    down = VMEM((L, U, *T3), F32)
    res = pl.pallas_call(
        functools.partial(up_kernel, count),
        out_shape=(HBM((HALF, OWN, CORES, *T3), BF), HBM((L, U, *T3), BF), *(HBM(a.shape, F32) for a in moments)),
        in_specs=[VM] * 3 + [HB] * 9,
        out_specs=(HB,) * 8,
        scratch_shapes=[VMEM((2, 2, BLOCK + 2 * Z, TILES, L, LANES), F32), down, down, VMEM((2, L, OWN, CORES, *T3), BF), VMEM((L, U, *T3), BF), DMA((9,)), DMA((9,))],
        compiler_params=pltpu.CompilerParams(vmem_limit_bytes=20 * 2**20),
        name="update",
    )(
        *(pltpu.with_memory_space_constraint(a, VMEM) for a in (Ggu, Gd, total)),
        *(pltpu.with_memory_space_constraint(a, HBM) for a in (view_gu(weights[0]), view_gu(weights[1]), view_d(weights[2]), *moments)),
    )
    unview = (unview_m, unview_m, lambda a: untiled(a, *m[2].shape[1:]))
    new = [f(a) for a, f in zip(res[2:], unview * 2)]
    return res[0], res[1], new[:3], new[3:]


AG_ORDER = ['Ax0_1+', 'Ax1_3++', 'By_0+', 'Cz_1+', 'Bo', 'Ay_2+', 'Co', 'Ao', 'Bz_2+', 'Ax0_2+', 'Ay_3+', 'Bx', 'Cy', 'By_1+', 'Cz_2+', 'Ax0_3+', 'Az_1', 'By_3+', 'Ax1_0+', 'Ay_0', 'Az_2', 'Cz_3+', 'Bz_1', 'Ax1_2+', 'Cx', 'Ay_1', 'Ax0_0+', 'By_2++', 'Az_3', 'Bz_3', 'Ax1_1+']


def ag_kernel(order, wgu, wd, VO, tmp, own_s, ex_ss, ex_rs, xs, ys, zis, zos, ds, dr, axr, ayr, azr, byr, bzr, bxr, czr, cxr, cyr):
    x, y, z, c = place()
    ox, oy, oc = 1 - x, 1 - y, 1 - c
    mid, sl, inner, end = line(z)
    NX, NY, NC, ZI, ZO = dev(ox, y, z, c), dev(x, oy, z, c), dev(x, y, z, oc), dev(x, y, inner, c), dev(x, y, end, c)
    zr = {'A': azr, 'B': bzr, 'C': czr}

    def task(name, p):
        n, axis, i = split(name)
        zz = sl[i]
        def at(idx): return VO.at[(p, *idx, PART[n], c)]
        def push(idx, to, ss, rs): remote(at(idx), at(idx), ss.at[p], rs, to).start()
        def give(idx): push(idx, NC, ds, dr.at[p])
        def chain(idx):
            rs = zr[n].at[p, zz]
            if i == 0: push(idx, ZI, zis, rs)
            @pl.when(mid)
            def _():
                if i == 1: push(idx, ZI, zis, rs)
                else: push(idx, ZO, zos, rs)
        if axis == 'o':
            here = x, y, z
            if n == 'A':
                chain(here)
                push(here, NY, ys, ayr.at[p, z])
                push(here, NX, xs, axr.at[p, z, 0])
            elif n == 'B': push(here, NX, xs, bxr.at[p])
            else: push(here, NY, ys, cyr.at[p])
            give(here)
        elif n == 'A':
            if axis == 'z':
                here = x, y, zz
                got(at(here), azr.at[p, zz])
                chain(here)
                push(here, NY, ys, ayr.at[p, zz])
                push(here, NX, xs, axr.at[p, zz, 0])
            elif axis == 'y':
                here = x, oy, zz
                got(at(here), ayr.at[p, zz])
                push(here, NX, xs, axr.at[p, zz, 1])
            else:
                k = int(name[2])
                here = ox, (oy if k else y), zz
                got(at(here), axr.at[p, zz, k])
            give(here)
        elif n == 'B':
            here, wide = (ox, y, z), (ALL, y, zz)
            if axis == 'y':
                here = ALL, oy, zz
                got(at(here), byr.at[p, zz])
            else:
                if axis == 'x': got(at(here), bxr.at[p])
                else:
                    here = wide
                    got(at(here), bzr.at[p, zz])
                chain(wide)
                push(wide, NY, ys, byr.at[p, zz])
            give(here)
        elif axis == 'y':
            here = x, oy, z
            got(at(here), cyr.at[p])
            push((x, ALL, z), NX, xs, cxr.at[p])
            give(here)
        else:
            here, wide = (ox, ALL, z), (ALL, ALL, zz)
            if axis == 'x': got(at(here), cxr.at[p])
            else:
                here = wide
                got(at(here), czr.at[p, zz])
            chain(wide)
            give(here)

    mine = VO.at[:, x, y, z]
    own = [copy(wd.at[l], mine.at[l, :, c], own_s.at[l]) for l in range(L)]
    own += [copy(wgu.at[q, pl.ds(c, Z), c], mine.at[L + q, pl.ds(OWN * c, Z), c], own_s.at[L + q]) for q in range(HALF)]
    own += [copy(wgu.at[:, Z * oc, c], tmp.at[0], own_s.at[NP])]
    for cp in own: cp.start()
    b = pltpu.get_barrier_semaphore()
    def signal(to): pl.semaphore_signal(b, 1, device_id=to, device_id_type=MESH)
    for to in (NX, NY, NC, ZI): signal(to)
    @pl.when(mid)
    def _(): signal(ZO)
    pl.semaphore_wait(b, 4 + mid.astype(jnp.int32))
    swap = [remote(wgu.at[q, pl.ds(c, Z), oc], mine.at[L + q, pl.ds(OWN * c, Z), oc], ex_ss.at[q], ex_rs.at[q], NC) for q in range(HALF)]
    swap += [remote(wgu.at[:, Z * oc, oc], tmp.at[1], ex_ss.at[HALF], ex_rs.at[HALF], NC)]
    for cp in swap: cp.start()
    for cp in own[:L]: cp.wait()

    def round_(r):
        @pl.when(r == 1)
        def _():
            for cp in own[L:] + swap: cp.wait()
            upper = lax.broadcasted_iota(jnp.int32, T3, 1) % SUB < Z
            first = upper.astype(jnp.int32) == oc
            for q in range(HALF):
                VO[L + q, x, y, z, Z, c] = jnp.where(first, tmp[0, q].astype(F32), tmp[1, q].astype(F32)).astype(BF)
        for n, lag in order:
            p = r - lag
            @pl.when((p >= 0) & (p < NP))
            def _(): task(n, p)
    over(NP + max(lag for _, lag in order), round_)

    def finish(p):
        q = VO.at[pl.ds(0, 5), 0, 0, 0, :, 0]
        got(q, xs.at[p])
        got(q, ys.at[p])
        @pl.when(mid)
        def _():
            got(q.at[:, pl.ds(0, 6)], zis.at[p])
            got(q, zos.at[p])
        @pl.when(jnp.logical_not(mid))
        def _(): got(q.at[:, pl.ds(0, 3)], zis.at[p])
        whole = VO.at[0, :, :, :, :, 0]
        got(whole, ds.at[p])
        got(whole, dr.at[p])
    over(NP, finish)


def place_kernel(VO, og, ou, od, sems):
    out = []
    def put(src, dst):
        out.append(copy(src, dst, sems.at[len(out)]))
        out[-1].start()
    for l in range(L):
        for i in range(X):
            for k in range(CORES): put(VO.at[l, i, :, :, :, k], od.at[l, i, :, :, k])
            put(VO.at[L + l, i], og.at[l, i])
            put(VO.at[2 * L + l, i], ou.at[l, i])
    for cp in out: cp.wait()


def ag_call(wgu, wd):
    four = DMA((NP, Z))
    one = DMA((NP,))
    VO = pl.pallas_call(
        functools.partial(ag_kernel, lagged(AG_ORDER)),
        out_shape=VMEM((NP, X, Y, Z, U, CORES, *T3), BF),
        in_specs=[HB] * 2,
        out_specs=VM,
        scratch_shapes=[VMEM((2, HALF, *T3), BF), DMA((NP + 1,)), DMA((HALF + 1,)), DMA((HALF + 1,))] + [one] * 6 + [DMA((NP, Z, 2)), four, four, four, four, one, four, one, one],
        compiler_params=pltpu.CompilerParams(collective_id=1, has_side_effects=True, vmem_limit_bytes=2**20),
        name="all_gather",
    )(*(pltpu.with_memory_space_constraint(a, HBM) for a in (wgu, wd)))
    G = jax.ShapeDtypeStruct((L, X, Y, Z, U, CORES, *T3), BF)
    D = jax.ShapeDtypeStruct((L, X, Y, Z, CORES, U, *T3), BF)
    og, ou, od = pl.pallas_call(
        place_kernel, out_shape=(G, G, D), in_specs=[VM], out_specs=(ANY,) * 3, scratch_shapes=[DMA((16,))],
        compiler_params=pltpu.CompilerParams(vmem_limit_bytes=2**20), name="place",
    )(pltpu.with_memory_space_constraint(VO, VMEM))
    return og, ou, od


def solution(mesh):
    def step(*arrays):
        terms, weights, m, v = (arrays[i : i + 3] for i in range(0, 12, 3))
        Ggu, Gd, total, _ = rs_call(terms[0][0], terms[1][0], terms[2][0])
        Wgu, Wd, m, v = up_call(Ggu, Gd, total, weights, m, v)
        whole = [untiled(a, *w.shape[1:]) for a, w in zip(ag_call(Wgu, Wd), weights)]
        return (*whole, *m, *v)

    all_of, cut = P(None, None, None), P(None, "dp", None)
    return jax.shard_map(
        step,
        mesh=mesh,
        in_specs=(P(("rep", "dp"), None, None, None),) * 3 + (all_of,) * 3 + (cut,) * 6,
        out_specs=(P("rep", None, None),) * 3 + (P("rep", "dp", None),) * 6,
        check_vma=False,
    )
```

```python
import functools

import jax
import jax.numpy as jnp
from jax import lax
from jax.experimental import pallas as pl
from jax.experimental.pallas import tpu as pltpu
from jax.sharding import PartitionSpec as P

MESH = pl.DeviceIdType.MESH
BF, F32 = jnp.bfloat16, jnp.float32
DMA = pltpu.SemaphoreType.DMA
VMEM, HBM = pltpu.VMEM, pltpu.HBM
ALL = slice(None)
L, X, Y, Z, U, CORES = 2, 2, 2, 4, 9, 2
N = X * Y * Z * CORES
SUB, ROWS, LANES = 8, 16, 128
T3 = (U, ROWS, LANES)
NP = 3 * L
HALF = NP - L
OWN = 5
PART = {'A': pl.ds(0, OWN), 'B': pl.ds(OWN, 3), 'C': U - 1}
BLOCK, TILES = 36, 36
RUN = TILES * L
MOMENTS = (2, 2, BLOCK + 2 * Z, TILES, L, LANES)
VM, HB, ANY = (pl.BlockSpec(memory_space=s) for s in (VMEM, HBM, pl.ANY))


def tiled(a):
    l, r, c = a.shape
    return a.reshape(l, r // SUB, SUB, c // LANES, LANES).swapaxes(2, 3)


def untiled(a, r, c):
    return a.reshape(L, r // SUB, c // LANES, SUB, LANES).swapaxes(2, 3).reshape(L, r, c)


def view_gu(g): return tiled(g).reshape(L, X, Y, Z, U, CORES, *T3)
def view_d(g): return tiled(g).reshape(L, X, Y, Z, CORES, U, *T3)


def place():
    d = lax.axis_index("dp")
    d, c = d // CORES, d % CORES
    d, z = d // Z, d % Z
    return d // Y, d % Y, z, c


def dev(x, y, z, c): return 0, ((x * Y + y) * Z + z) * CORES + c


def line(z):
    h = z // 2
    return (z == 1) | (z == 2), [z, 1 - z + Z * h, 2 - h, 3 - 3 * h], z + 1 - 2 * h, 3 * h


def over(n, f): lax.fori_loop(0, n, lambda i, _: (f(i), 0)[1], 0)


def copy(src, dst, sem): return pltpu.make_async_copy(src, dst, sem)


def remote(src, dst, ss, rs, to): return pltpu.make_async_remote_copy(src, dst, ss, rs, device_id=to, device_id_type=MESH)


def got(ref, sem): copy(ref, ref, sem).wait()


def greet(barrier, to, mid, too):
    def signal(one): pl.semaphore_signal(barrier, 1, device_id=one, device_id_type=MESH)
    for one in to: signal(one)
    @pl.when(mid)
    def _(): signal(too)
    pl.semaphore_wait(barrier, len(to) + mid.astype(jnp.int32))


def pinned(a, space): return pltpu.with_memory_space_constraint(a, space)


def split(name): return name[0], name[1], int(name[-1]) if name[-1].isdigit() else 0


def lagged(names): return [(n.rstrip('+'), n.count('+')) for n in names]


RS_ORDER = ['By0', 'Ax0', 'Ax7+', 'Cz0', 'By2', 'Bf++', 'Az1+', 'Ax1', 'Ax4', 'Cz1', 'By1', 'Ax2', 'Cz2', 'Ax6', 'Ax5', 'Bx+', 'Ay0', 'Bz0', 'Ay1', 'Bz2', 'Ax3', 'By3', 'Bz1', 'Ay2', 'Az0', 'Cx', 'Ay3+', 'Az2+', 'Af++', 'Cf++', 'Cy+']
TURN = 24
CLASSES = {
    'A': ((OWN,), ['Ax0', 'Ax1', 'Ax2', 'Ax3', 'Ax4', 'Ax5', 'Ax6', 'Ax7', 'Ay0', 'Ay1', 'Ay2', 'Ay3', 'Az0', 'Az1', 'Az2', 'Af']),
    'By': ((X, 3), ['By0', 'By1', 'By2', 'By3', 'Bz0', 'Bz1', 'Bz2']),
    'Bx': ((3,), ['Bx', 'Bf']),
    'Cz': ((X, Y), ['Cz0', 'Cz1', 'Cz2']),
    'Cx': ((Y,), ['Cx']),
    'Cy': ((), ['Cy', 'Cf']),
}
CLASS_OF = {n: (k, i) for k, (_, names) in CLASSES.items() for i, n in enumerate(names)}
ARRIVE = {'Ax': (8, 'A'), 'Ay': (Z, 'A'), 'Az': (5, 'A'), 'By': (Z, 'By'), 'Bz': (5, 'By'), 'Bx': (1, 'Bx'), 'Cz': (5, 'Cz'), 'Cx': (1, 'Cx'), 'Cy': (1, 'Cy')}
LAST, CROSS = 2, 4


def rs_kernel(order, gg, gu, gd, *refs):
    moments, (Ggu, Gd, TOT, MOM, DOWN, PARTNER), scr = refs[:6], refs[6:12], iter(refs[12:])
    take = lambda names: {n: next(scr) for n in names}
    own, par, snd, rcv = take(CLASSES), take(CLASSES), take(CLASSES), take(ARRIVE)
    fin, acc, sall = take(range(3)).values()
    own_s, par_s, snd_s, first_s, rcv_s = take(CLASSES), take(CLASSES), take(CLASSES), take(CLASSES), take(ARRIVE)
    d2d_ss, d2d_rs, gx_ss, gx_rs, sa_ss, sa_rs, mom_s = take(range(7)).values()
    x, y, z, c = place()
    ox, oy, oc = 1 - x, 1 - y, 1 - c
    me = lax.axis_index("dp")
    mid, near, inner, end = line(z)
    zo = near[::-1]
    side = z + 1 - 2 * (z % 2)
    NX, NY, NC = dev(ox, y, z, c), dev(x, oy, z, c), dev(x, y, z, oc)

    def block(name):
        n, axis, i = split(name)
        u = PART[n]
        if axis == 'f': return x, y, z, u
        if n == 'A':
            if axis == 'x': return ox, (oy if i < Z else y), zo[i % Z], u
            return x, (oy if axis == 'y' else y), zo[i], u
        if n == 'B':
            if axis == 'x': return ox, y, z, u
            return ALL, (oy if axis == 'y' else y), zo[i], u
        return {'z': (ALL, ALL, zo[i], u), 'x': (ox, ALL, z, u), 'y': (x, oy, z, u)}[axis]

    def cut(k, l, b, core):
        return gd.at[(l, *b[:3], core, b[3])] if k == 2 else (gg, gu)[k].at[(l, *b, core)]

    def reload(name, p):
        cl, i = CLASS_OF[name]
        b = block(name)
        @pl.when((p >= 0) & (p < NP))
        def _():
            for k in range(3):
                @pl.when(p // L == k)
                def _(): copy(cut(k, p % L, b, c), own[cl].at[i], own_s[cl].at[i]).start()
            @pl.when(p > 0)
            def _(): copy(PARTNER.at[(p, *b)], par[cl].at[i], par_s[cl].at[i]).start()

    def send(name, p):
        cl, i = CLASS_OF[name]
        n, axis, j = split(name)
        if axis == 'x': to, slot = NX, j
        elif axis == 'y': to, slot = NY, j
        elif j < 2: to, slot = dev(x, y, inner, c), j + 3 * mid.astype(jnp.int32)
        else: to, slot = dev(x, y, side, c), LAST
        kind = name[:2]
        return remote(snd[cl].at[i], rcv[kind].at[p, slot], snd_s[cl].at[i], rcv_s[kind].at[p, slot], to)

    def add(dst, refs, lead, last):
        def one(*idx):
            at = idx if idx else ...
            t = sum(r[at].astype(F32) for r in refs).astype(BF)
            dst[at] = t
            if last:
                t = t.astype(F32)
                acc[...] += jnp.sum(t * t, axis=0)
        if not lead: one()
        elif len(lead) == 1: over(lead[0], one)
        else: over(lead[0], lambda i: over(lead[1], lambda j: one(i, j)))

    def task(name, p):
        cl, i = CLASS_OF[name]
        n, axis, j = split(name)
        lead = CLASSES[cl][0]
        R = lambda kind, s: rcv[kind].at[p, s]
        def arrive(*which):
            for kind, s in which: got(R(kind, s), rcv_s[kind].at[p, s])
        got(own[cl].at[i], own_s[cl].at[i])
        got(par[cl].at[i], par_s[cl].at[i])
        zk, refs, far, wait, farwait = n + 'z', [], [], [], []
        if axis == 'z':
            s = (0, 1, 3)[j]
            far, farwait = [R(zk, s)], [(zk, s)]
            wait = {'A': [('Ax', Z + j), ('Ay', j)], 'B': [('By', j)], 'C': []}[n]
            refs = [R(*w) for w in wait]
        elif name[:2] == 'Ay':
            wait = [('Ax', j)]
            refs = [R(*w) for w in wait]
        elif name == 'Af':
            wait, farwait = [('Ax', Z + 3), ('Ay', 3), (zk, LAST)], [(zk, CROSS)]
            refs, far = [R(*w) for w in wait], [R(zk, CROSS)]
        elif axis != 'y' or n == 'C':
            if n == 'B' and axis == 'x' or n == 'C' and axis == 'x': wait, farwait = [(zk, LAST)], [(zk, CROSS)]
            if name == 'Bx': wait += [('By', 3)]
            if name in ('Bf', 'Cy'): wait = [(n + 'x', 0)]
            if name == 'Cf': wait = [('Cy', 0)]
            here = {'Bx': (ox,), 'Bf': (x,), 'Cx': (ox,), 'Cy': (x, oy), 'Cf': (x, y)}.get(name)
            if here:
                refs, far = [R(zk, LAST).at[here]], [R(zk, CROSS).at[here]]
                if n == 'B': refs += [R('By', 3).at[here]]
                if name == 'Bf': refs += [R('Bx', 0)]
                if name == 'Cy': refs += [R('Cx', 0).at[oy]]
                if name == 'Cf': refs += [R('Cx', 0).at[y], R('Cy', 0)]
        arrive(*wait)
        last = axis == 'f'
        if last: dst = fin.at[p, PART[n]]
        else:
            @pl.when(p > 0)
            def _(): send(name, p).wait_send()
            dst = snd[cl].at[i]
        refs = [own[cl].at[i], par[cl].at[i]] + refs
        if far:
            @pl.when(mid)
            def _():
                arrive(*farwait)
                add(dst, refs + far, lead, last)
            @pl.when(jnp.logical_not(mid))
            def _(): add(dst, refs, lead, last)
        else: add(dst, refs, lead, last)
        if not last: send(name, p).start()

    def swap0(name):
        cl, i = CLASS_OF[name]
        return remote(cut(0, 0, block(name), oc), par[cl].at[i], first_s[cl].at[i], par_s[cl].at[i], NC)

    def swap(p):
        parts = [(ox, ALL, ALL, PART['A']), (ALL, ALL, ALL, PART['B']), (ALL, ALL, ALL, PART['C']), (x, ALL, ALL, PART['A'])]
        return [remote(cut(p // L, p % L, q, oc), PARTNER.at[(p, *q)], d2d_ss.at[p, i], d2d_rs.at[p, i], NC) for i, q in enumerate(parts)]

    acc[...] = jnp.zeros_like(acc)
    for n, _ in order: reload(n, jnp.int32(0))
    b = pltpu.get_barrier_semaphore()
    def others(f):
        def one(i):
            @pl.when(i != me)
            def _(): f((0, i))
        over(N, one)
    greet(b, (NX, NY, NC, dev(x, y, inner, c)), mid, dev(x, y, end, c))
    for n, _ in sorted(order, key=lambda t: t[1]): swap0(n).start()
    for p in range(1, NP):
        for cp in swap(p): cp.start()

    finlag = max(lag for n, lag in order if n[1] == 'f')
    def rows(p): return remote(fin.at[p, pl.ds(Z * oc, OWN)], Ggu.at[p // L, p % L, :, c], gx_ss.at[p], gx_rs.at[p], NC)
    early = [copy(moments[k + 3 * i], MOM.at[k, i, pl.ds(Z, BLOCK)], mom_s.at[k, i]) for k in range(2) for i in range(2)]
    early += [copy(moments[2 + 3 * i], DOWN.at[i], mom_s.at[2, i]) for i in range(2)]
    def round_(r):
        @pl.when(r == 1)
        def _():
            for cp in early: cp.start()
        for i, (n, lag) in enumerate(order):
            p = r - lag
            @pl.when((p >= 0) & (p < NP))
            def _(): task(n, p)
            if i == TURN:
                for q in range(1, NP):
                    @pl.when(q == r + 1)
                    def _():
                        for cp in swap(q): cp.wait_recv()
                for m, ml in order[:TURN]:
                    @pl.when(r >= ml)
                    def _(): reload(m, r - ml + 1)
            if i >= TURN:
                @pl.when(p >= 0)
                def _(): reload(n, p + 1)
        q = r - finlag
        @pl.when((q >= 0) & (q < HALF))
        def _(): rows(q).start()
    over(NP + max(lag for _, lag in order), round_)

    sall[me] = acc[0:SUB] + acc[SUB:ROWS]
    others(lambda to: remote(sall.at[me], sall.at[me], sa_ss, sa_rs, to).start())
    for l in range(L): Gd[l] = fin[HALF + l]
    for k in range(2):
        for i in range(2):
            for at in (0, Z + BLOCK): MOM[k, i, at:at + Z] = jnp.zeros((Z, TILES, L, LANES), F32)
    for cp in early: cp.wait()
    for p in range(HALF):
        k, l = p // L, p % L
        Ggu[k, l, :, c] = fin[p, pl.ds(Z * c, OWN)]
        rows(p).wait()
    for n, lag in order:
        swap0(n).wait_send()
        if n[1] != 'f': send(n, NP - 1).wait_send()
    for p in range(1, NP):
        for cp in swap(p): cp.wait_send()
    rest = sall.at[pl.ds(0, N - 1)]
    got(rest, sa_rs)
    got(rest, sa_ss)
    TOT[...] = jnp.sum(sall[...], axis=0)


def rs_call(gg, gu, gd, moments):
    bufs = [VMEM((len(names), *shape, *T3), BF) for shape, names in CLASSES.values()]
    sems = [DMA((len(names),)) for _, names in CLASSES.values()]
    scratch = bufs * 3 + [VMEM((NP, n, *CLASSES[cl][0], *T3), BF) for n, cl in ARRIVE.values()]
    scratch += [VMEM((NP, U, *T3), BF), VMEM((ROWS, LANES), F32), VMEM((N, SUB, LANES), F32)]
    scratch += sems * 4 + [DMA((NP, n)) for n, _ in ARRIVE.values()]
    scratch += [DMA((NP, 4)), DMA((NP, 4)), DMA((HALF,)), DMA((HALF,)), DMA(()), DMA(()), DMA((3, 2))]
    return pl.pallas_call(
        functools.partial(rs_kernel, lagged(RS_ORDER)),
        out_shape=(VMEM((2, L, OWN, CORES, *T3), BF), VMEM((L, U, *T3), BF), VMEM((SUB, LANES), F32), VMEM(MOMENTS, F32), VMEM((2, L, U, *T3), F32), HBM((NP, X, Y, Z, U, *T3), BF)),
        in_specs=[HB] * 9,
        out_specs=(VM, VM, VM, VM, VM, HB),
        scratch_shapes=scratch,
        compiler_params=pltpu.CompilerParams(collective_id=0, has_side_effects=True, vmem_limit_bytes=53 * 2**20),
        name="reduce_scatter",
    )(*(pinned(a, HBM) for a in (view_gu(gg), view_gu(gu), view_d(gd), *moments)))


def up_kernel(count, Ggu, Gd, TOT, MOM, DOWN, wg, wu, wd, Wgu, Wd, *refs):
    new, (mom, down, wb, wdb, ld, st, ds) = refs[:6], refs[6:]
    x, y, z, c = place()
    loads = [copy(wd.at[:, x, y, z, c], wdb, ld.at[2])]
    loads += [copy((wg, wu)[k].at[:, x, y, z, pl.ds(Z * c, OWN)], wb.at[k], ld.at[k]) for k in range(2)]
    for cp in loads: cp.start()
    stores = []
    def store(src, dst):
        stores.append(copy(src, dst, st.at[len(stores)]))
        stores[-1].start()
    s = jnp.sum(jnp.sum(TOT[...], axis=0, keepdims=True), axis=1, keepdims=True)
    factor = jnp.minimum(1.0, 0.5 * lax.rsqrt(s * (1.0 / count) + 1e-30))
    def adamw(w, m, v, g):
        g = g * factor
        m = 0.9 * m + 0.1 * g
        v = 0.95 * v + 0.05 * g * g
        return w - 0.02 * (m * lax.rsqrt(v + 1e-8) + 0.1 * w), m, v
    rows = pl.ds(Z, BLOCK)
    for k in range(2):
        loads[1 + k].wait()
        flat = lambda ref, i: ref.at[k, i].reshape((BLOCK + 2 * Z) * RUN, LANES)
        M, V, newM, newV = flat(MOM, 0), flat(MOM, 1), flat(mom, 0), flat(mom, 1)
        def tile(l, u, ch):
            base = (SUB * u + Z - Z * c) * RUN + TILES * ch + l
            for j in range(U):
                g, w = Ggu[k, l, u, ch, j].astype(F32), wb[k, l, u, ch, j].astype(F32)
                half = []
                for e in range(2):
                    at = pl.ds(base + (2 * j + e) * L, SUB, stride=RUN)
                    h = slice(SUB * e, SUB * e + SUB)
                    wn, newM[at, :], newV[at, :] = adamw(w[h], M[at, :], V[at, :], g[h])
                    half.append(wn)
                wb[k, l, u, ch, j] = jnp.concatenate(half).astype(BF)
        over(L, lambda l: over(OWN, lambda u: over(CORES, lambda ch: tile(l, u, ch))))
        store(wb.at[k], Wgu.at[pl.ds(L * k, L)])
        for i in range(2): store(mom.at[k, i, rows], new[k + 3 * i])
    loads[0].wait()
    def layer(l):
        def unit(u):
            for j in range(U):
                at = (l, u, j)
                w, m, v = adamw(wdb[at].astype(F32), DOWN[(0, *at)], DOWN[(1, *at)], Gd[at].astype(F32))
                wdb[at] = w.astype(BF)
                down[(0, *at)], down[(1, *at)] = m, v
        over(U, unit)
        for i in range(2): copy(down.at[i, l], new[2 + 3 * i].at[l], ds.at[i, l]).start()
    over(L, layer)
    store(wdb, Wd)
    for cp in stores: cp.wait()
    for l in range(L):
        for i in range(2): copy(down.at[i, l], new[2 + 3 * i].at[l], ds.at[i, l]).wait()


def view_m(m): return m.reshape(L, BLOCK, TILES, LANES).transpose(1, 2, 0, 3)
def unview_m(m): return m.transpose(2, 0, 1, 3).reshape(L, BLOCK, TILES * LANES)
def view_md(m): return tiled(m).reshape(L, U, *T3)


def up_call(Ggu, Gd, total, MOM, DOWN, weights, moments):
    count = sum(w.size for w in weights)
    W, Wd = (HALF, OWN, CORES, *T3), (L, U, *T3)
    res = pl.pallas_call(
        functools.partial(up_kernel, count),
        out_shape=(HBM(W, BF), HBM(Wd, BF), *(HBM(a.shape, F32) for a in moments)),
        in_specs=[VM] * 5 + [HB] * 3,
        out_specs=[HB] * 8,
        scratch_shapes=[VMEM(MOMENTS, F32), VMEM((2, *Wd), F32), VMEM((2, L, *W[1:]), BF), VMEM(Wd, BF), DMA((3,)), DMA((7,)), DMA((2, L))],
        compiler_params=pltpu.CompilerParams(vmem_limit_bytes=20 * 2**20),
        name="update",
    )(
        *(pinned(a, VMEM) for a in (Ggu, Gd, total, MOM, DOWN)),
        *(pinned(f(w), HBM) for f, w in zip((view_gu, view_gu, view_d), weights)),
    )
    rows, columns = weights[2].shape[1:]
    unview = (unview_m, unview_m, lambda a: untiled(a, rows // N, columns))
    new = [f(a) for a, f in zip(res[2:], unview * 2)]
    return res[0], res[1], new


AG_ORDER = ['Ax0_1+', 'Ax1_3++', 'By_0+', 'Cz_1+', 'Bo', 'Ay_2+', 'Co', 'Ao', 'Bz_2+', 'Ax0_2+', 'Ay_3+', 'Bx', 'Cy', 'By_1+', 'Cz_2+', 'Ax0_3+', 'Az_1', 'By_3+', 'Ax1_0+', 'Ay_0', 'Az_2', 'Cz_3+', 'Bz_1', 'Ax1_2+', 'Cx', 'Ay_1', 'Ax0_0+', 'By_2++', 'Az_3', 'Bz_3', 'Ax1_1+']


def ag_kernel(order, wgu, wd, VO, tmp, own_s, ex_ss, ex_rs, xs, ys, zis, zos, ds, dr, axr, ayr, azr, byr, bzr, bxr, czr, cxr, cyr):
    x, y, z, c = place()
    ox, oy, oc = 1 - x, 1 - y, 1 - c
    mid, sl, inner, end = line(z)
    NX, NY, NC, ZI, ZO = dev(ox, y, z, c), dev(x, oy, z, c), dev(x, y, z, oc), dev(x, y, inner, c), dev(x, y, end, c)
    zr = {'A': azr, 'B': bzr, 'C': czr}

    def task(name, p):
        n, axis, i = split(name)
        zz = sl[i]
        def at(idx): return VO.at[(p, *idx, PART[n], c)]
        def push(idx, to, ss, rs): remote(at(idx), at(idx), ss.at[p], rs, to).start()
        def give(idx): push(idx, NC, ds, dr.at[p])
        def chain(idx):
            rs = zr[n].at[p, zz]
            if i == 0: push(idx, ZI, zis, rs)
            @pl.when(mid)
            def _():
                if i == 1: push(idx, ZI, zis, rs)
                else: push(idx, ZO, zos, rs)
        if axis == 'o':
            here = x, y, z
            if n == 'A':
                chain(here)
                push(here, NY, ys, ayr.at[p, z])
                push(here, NX, xs, axr.at[p, z, 0])
            elif n == 'B': push(here, NX, xs, bxr.at[p])
            else: push(here, NY, ys, cyr.at[p])
            give(here)
        elif n == 'A':
            if axis == 'z':
                here = x, y, zz
                got(at(here), azr.at[p, zz])
                chain(here)
                push(here, NY, ys, ayr.at[p, zz])
                push(here, NX, xs, axr.at[p, zz, 0])
            elif axis == 'y':
                here = x, oy, zz
                got(at(here), ayr.at[p, zz])
                push(here, NX, xs, axr.at[p, zz, 1])
            else:
                k = int(name[2])
                here = ox, (oy if k else y), zz
                got(at(here), axr.at[p, zz, k])
            give(here)
        elif n == 'B':
            here, wide = (ox, y, z), (ALL, y, zz)
            if axis == 'y':
                here = ALL, oy, zz
                got(at(here), byr.at[p, zz])
            else:
                if axis == 'x': got(at(here), bxr.at[p])
                else:
                    here = wide
                    got(at(here), bzr.at[p, zz])
                chain(wide)
                push(wide, NY, ys, byr.at[p, zz])
            give(here)
        elif axis == 'y':
            here = x, oy, z
            got(at(here), cyr.at[p])
            push((x, ALL, z), NX, xs, cxr.at[p])
            give(here)
        else:
            here, wide = (ox, ALL, z), (ALL, ALL, zz)
            if axis == 'x': got(at(here), cxr.at[p])
            else:
                here = wide
                got(at(here), czr.at[p, zz])
            chain(wide)
            give(here)

    mine = VO.at[:, x, y, z]
    own = [copy(wd.at[l], mine.at[l, :, c], own_s.at[l]) for l in range(L)]
    own += [copy(wgu.at[q, pl.ds(c, Z), c], mine.at[L + q, pl.ds(OWN * c, Z), c], own_s.at[L + q]) for q in range(HALF)]
    own += [copy(wgu.at[:, Z * oc, c], tmp.at[0], own_s.at[NP])]
    for cp in own: cp.start()
    greet(pltpu.get_barrier_semaphore(), (NX, NY, NC, ZI), mid, ZO)
    swap = [remote(wgu.at[q, pl.ds(c, Z), oc], mine.at[L + q, pl.ds(OWN * c, Z), oc], ex_ss.at[q], ex_rs.at[q], NC) for q in range(HALF)]
    swap += [remote(wgu.at[:, Z * oc, oc], tmp.at[1], ex_ss.at[HALF], ex_rs.at[HALF], NC)]
    for cp in swap: cp.start()
    for cp in own[:L]: cp.wait()

    def round_(r):
        @pl.when(r == 1)
        def _():
            for cp in own[L:] + swap: cp.wait()
            upper = lax.broadcasted_iota(jnp.int32, T3, 1) % SUB < Z
            first = upper.astype(jnp.int32) == oc
            for q in range(HALF):
                VO[L + q, x, y, z, Z, c] = jnp.where(first, tmp[0, q].astype(F32), tmp[1, q].astype(F32)).astype(BF)
        for n, lag in order:
            p = r - lag
            @pl.when((p >= 0) & (p < NP))
            def _(): task(n, p)
    over(NP + max(lag for _, lag in order), round_)

    def finish(p):
        q = VO.at[pl.ds(0, 5), 0, 0, 0, :, 0]
        got(q, xs.at[p])
        got(q, ys.at[p])
        @pl.when(mid)
        def _():
            got(q.at[:, pl.ds(0, 6)], zis.at[p])
            got(q, zos.at[p])
        @pl.when(jnp.logical_not(mid))
        def _(): got(q.at[:, pl.ds(0, 3)], zis.at[p])
        whole = VO.at[0, :, :, :, :, 0]
        got(whole, ds.at[p])
        got(whole, dr.at[p])
    over(NP, finish)


def place_kernel(VO, og, ou, od, sems):
    out = []
    def put(src, dst):
        out.append(copy(src, dst, sems.at[len(out)]))
        out[-1].start()
    for l in range(L):
        for i in range(X):
            for k in range(CORES): put(VO.at[l, i, :, :, :, k], od.at[l, i, :, :, k])
            put(VO.at[L + l, i], og.at[l, i])
            put(VO.at[2 * L + l, i], ou.at[l, i])
    for cp in out: cp.wait()


def ag_call(wgu, wd):
    four = DMA((NP, Z))
    one = DMA((NP,))
    VO = pl.pallas_call(
        functools.partial(ag_kernel, lagged(AG_ORDER)),
        out_shape=VMEM((NP, X, Y, Z, U, CORES, *T3), BF),
        in_specs=[HB] * 2,
        out_specs=VM,
        scratch_shapes=[VMEM((2, HALF, *T3), BF), DMA((NP + 1,)), DMA((HALF + 1,)), DMA((HALF + 1,))] + [one] * 6 + [DMA((NP, Z, 2)), four, four, four, four, one, four, one, one],
        compiler_params=pltpu.CompilerParams(collective_id=1, has_side_effects=True, vmem_limit_bytes=2**20),
        name="all_gather",
    )(pinned(wgu, HBM), pinned(wd, HBM))
    G = jax.ShapeDtypeStruct((L, X, Y, Z, U, CORES, *T3), BF)
    D = jax.ShapeDtypeStruct((L, X, Y, Z, CORES, U, *T3), BF)
    og, ou, od = pl.pallas_call(
        place_kernel, out_shape=(G, G, D), in_specs=[VM], out_specs=(ANY,) * 3, scratch_shapes=[DMA((16,))],
        compiler_params=pltpu.CompilerParams(vmem_limit_bytes=2**20), name="place",
    )(pinned(VO, VMEM))
    return og, ou, od


def solution(mesh):
    def step(*arrays):
        terms, weights, m, v = (arrays[i : i + 3] for i in range(0, 12, 3))
        moments = [f(a) for a, f in zip((*m, *v), (view_m, view_m, view_md) * 2)]
        sums = rs_call(*(t[0] for t in terms), moments)
        Wgu, Wd, new = up_call(*sums[:5], weights, moments)
        whole = [untiled(a, *w.shape[1:]) for a, w in zip(ag_call(Wgu, Wd), weights)]
        return (*whole, *new)

    all_of, cut = P(None, None, None), P(None, "dp", None)
    return jax.shard_map(
        step,
        mesh=mesh,
        in_specs=(P(("rep", "dp"), None, None, None),) * 3 + (all_of,) * 3 + (cut,) * 6,
        out_specs=(P("rep", None, None),) * 3 + (P("rep", "dp", None),) * 6,
        check_vma=False,
    )
```

```python
import functools

import jax
import jax.numpy as jnp
from jax import lax
from jax.experimental import pallas as pl
from jax.experimental.pallas import tpu as pltpu
from jax.sharding import PartitionSpec as P

MESH = pl.DeviceIdType.MESH
BF, F32 = jnp.bfloat16, jnp.float32
DMA = pltpu.SemaphoreType.DMA
VMEM, HBM = pltpu.VMEM, pltpu.HBM
ALL = slice(None)
L, X, Y, Z, U, CORES = 2, 2, 2, 4, 9, 2
N = X * Y * Z * CORES
SUB, ROWS, LANES = 8, 16, 128
T3 = (U, ROWS, LANES)
NP = 3 * L
HALF = NP - L
OWN = 5
PART = {'A': pl.ds(0, OWN), 'B': pl.ds(OWN, 3), 'C': U - 1}
BLOCK, TILES = 36, 36
RUN = TILES * L
MOMENTS = (2, 2, OWN * SUB, TILES, L, LANES)
VM, HB, ANY = (pl.BlockSpec(memory_space=s) for s in (VMEM, HBM, pl.ANY))


def tiled(a):
    l, r, c = a.shape
    return a.reshape(l, r // SUB, SUB, c // LANES, LANES).swapaxes(2, 3)


def untiled(a, r, c):
    return a.reshape(L, r // SUB, c // LANES, SUB, LANES).swapaxes(2, 3).reshape(L, r, c)


def view_gu(g): return tiled(g).reshape(L, X, Y, Z, U, CORES, *T3)
def view_d(g): return tiled(g).reshape(L, X, Y, Z, CORES, U, *T3)


def place():
    d = lax.axis_index("dp")
    d, c = d // CORES, d % CORES
    d, z = d // Z, d % Z
    return d // Y, d % Y, z, c


def dev(x, y, z, c): return 0, ((x * Y + y) * Z + z) * CORES + c


def line(z):
    h = z // 2
    return (z == 1) | (z == 2), [z, 1 - z + Z * h, 2 - h, 3 - 3 * h], z + 1 - 2 * h, 3 * h


def over(n, f): lax.fori_loop(0, n, lambda i, _: (f(i), 0)[1], 0)


def copy(src, dst, sem): return pltpu.make_async_copy(src, dst, sem)


def remote(src, dst, ss, rs, to): return pltpu.make_async_remote_copy(src, dst, ss, rs, device_id=to, device_id_type=MESH)


def got(ref, sem): copy(ref, ref, sem).wait()


def greet(to, mid, too):
    barrier = pltpu.get_barrier_semaphore()
    def signal(one): pl.semaphore_signal(barrier, 1, device_id=one, device_id_type=MESH)
    for one in to: signal(one)
    @pl.when(mid)
    def _(): signal(too)
    return lambda: pl.semaphore_wait(barrier, len(to) + mid.astype(jnp.int32))


def pinned(a, space): return pltpu.with_memory_space_constraint(a, space)


def split(name): return name[0], name[1], int(name[-1]) if name[-1].isdigit() else 0


def lagged(orders): return [[(n.rstrip('+'), n.count('+')) for n in names] for names in orders]


RS_ORDER = [
    ['Cz0', 'By0', 'Ax0', 'Cz2', 'Az0+', 'By1', 'Cz1', 'Ay1+', 'Ax4', 'Ax5', 'Ay3++', 'Az2++', 'By2', 'Bz0', 'Cy++', 'Ay2+', 'Az1+', 'Ax1', 'Ay0', 'Bx++', 'Ax2', 'By3+', 'Ax6+', 'Cx+', 'Ax7+', 'Af++', 'Bz1', 'Bz2+', 'Cf++', 'Ax3', 'Bf++'],
    ['Cz1+', 'Cz2+', 'By1', 'Ax0', 'Ax1', 'Ay2+', 'Ax7++', 'Az1++', 'By0', 'Ax2', 'Ay0', 'Bz1+', 'Az2++', 'Cz0', 'Cy++', 'Ax4', 'Ax3', 'Bx++', 'By3+', 'Ax6+', 'By2', 'Bz2+', 'Az0+', 'Ax5', 'Ay1', 'Ay3+', 'Cx+', 'Bz0', 'Af++', 'Cf++', 'Bf++'],
]
AHEAD = 5
CLASSES = {
    'A': ((OWN,), ['Ax0', 'Ax1', 'Ax2', 'Ax3', 'Ax4', 'Ax5', 'Ax6', 'Ax7', 'Ay0', 'Ay1', 'Ay2', 'Ay3', 'Az0', 'Az1', 'Az2', 'Af']),
    'By': ((X, 3), ['By0', 'By1', 'By2', 'By3', 'Bz0', 'Bz1', 'Bz2']),
    'Bx': ((3,), ['Bx', 'Bf']),
    'Cz': ((X, Y), ['Cz0', 'Cz1', 'Cz2']),
    'Cx': ((Y,), ['Cx']),
    'Cy': ((), ['Cy', 'Cf']),
}
CLASS_OF = {n: (k, i) for k, (_, names) in CLASSES.items() for i, n in enumerate(names)}
ARRIVE = {'Ax': (8, 'A'), 'Ay': (Z, 'A'), 'Az': (5, 'A'), 'By': (Z, 'By'), 'Bz': (5, 'By'), 'Bx': (1, 'Bx'), 'Cz': (5, 'Cz'), 'Cx': (1, 'Cx'), 'Cy': (1, 'Cy')}
LAST, CROSS = 2, 4


def rs_kernel(orders, gg, gu, gd, wg, wu, *refs):
    moments, (Ggu, Gd, TOT, MOM, DOWN, WGU, PARTNER), scr = refs[:6], refs[6:13], iter(refs[13:])
    take = lambda names: {n: next(scr) for n in names}
    own, par, snd, rcv = take(CLASSES), take(CLASSES), take(CLASSES), take(ARRIVE)
    fin, acc, sall = take(range(3)).values()
    own_s, par_s, snd_s, first_s, rcv_s = take(CLASSES), take(CLASSES), take(CLASSES), take(CLASSES), take(ARRIVE)
    d2d_ss, d2d_rs, gx_ss, gx_rs, sa_ss, sa_rs, mom_s = take(range(7)).values()
    x, y, z, c = place()
    ox, oy, oc = 1 - x, 1 - y, 1 - c
    me = lax.axis_index("dp")
    mid, near, inner, end = line(z)
    zo = near[::-1]
    side = z + 1 - 2 * (z % 2)
    NX, NY, NC = dev(ox, y, z, c), dev(x, oy, z, c), dev(x, y, z, oc)

    def block(name):
        n, axis, i = split(name)
        u = PART[n]
        if axis == 'f': return x, y, z, u
        if n == 'A':
            if axis == 'x': return ox, (oy if i < Z else y), zo[i % Z], u
            return x, (oy if axis == 'y' else y), zo[i], u
        if n == 'B':
            if axis == 'x': return ox, y, z, u
            return ALL, (oy if axis == 'y' else y), zo[i], u
        return {'z': (ALL, ALL, zo[i], u), 'x': (ox, ALL, z, u), 'y': (x, oy, z, u)}[axis]

    def cut(k, l, b, core):
        return gd.at[(l, *b[:3], core, b[3])] if k == 2 else (gg, gu)[k].at[(l, *b, core)]

    def reload(name, p):
        cl, i = CLASS_OF[name]
        b = block(name)
        @pl.when((p >= 0) & (p < NP))
        def _():
            for k in range(3):
                @pl.when(p // L == k)
                def _(): copy(cut(k, p % L, b, c), own[cl].at[i], own_s[cl].at[i]).start()
            @pl.when(p > 0)
            def _(): copy(PARTNER.at[(p, *b)], par[cl].at[i], par_s[cl].at[i]).start()

    def send(name, p, middle):
        cl, i = CLASS_OF[name]
        n, axis, j = split(name)
        if axis == 'x': to, slot = NX, j
        elif axis == 'y': to, slot = NY, j
        elif j < 2: to, slot = dev(x, y, inner, c), j + 3 * middle
        else: to, slot = dev(x, y, side, c), LAST
        kind = name[:2]
        return remote(snd[cl].at[i], rcv[kind].at[p, slot], snd_s[cl].at[i], rcv_s[kind].at[p, slot], to)

    def add(dst, refs, lead, last):
        def one(*idx):
            at = idx if idx else ...
            t = sum(r[at].astype(F32) for r in refs).astype(BF)
            dst[at] = t
            if last:
                t = t.astype(F32)
                acc[...] += jnp.sum(t * t, axis=0)
        if not lead: one()
        elif len(lead) == 1: over(lead[0], one)
        else: over(lead[0], lambda i: over(lead[1], lambda j: one(i, j)))

    def task(name, p, middle):
        cl, i = CLASS_OF[name]
        n, axis, j = split(name)
        lead = CLASSES[cl][0]
        R = lambda kind, s: rcv[kind].at[p, s]
        def arrive(*which):
            for kind, s in which: got(R(kind, s), rcv_s[kind].at[p, s])
        got(own[cl].at[i], own_s[cl].at[i])
        got(par[cl].at[i], par_s[cl].at[i])
        zk, refs, far, wait, farwait = n + 'z', [], [], [], []
        if axis == 'z':
            s = (0, 1, 3)[j]
            far, farwait = [R(zk, s)], [(zk, s)]
            wait = {'A': [('Ax', Z + j), ('Ay', j)], 'B': [('By', j)], 'C': []}[n]
            refs = [R(*w) for w in wait]
        elif name[:2] == 'Ay':
            wait = [('Ax', j)]
            refs = [R(*w) for w in wait]
        elif name == 'Af':
            wait, farwait = [('Ax', Z + 3), ('Ay', 3), (zk, LAST)], [(zk, CROSS)]
            refs, far = [R(*w) for w in wait], [R(zk, CROSS)]
        elif axis != 'y' or n == 'C':
            if n == 'B' and axis == 'x' or n == 'C' and axis == 'x': wait, farwait = [(zk, LAST)], [(zk, CROSS)]
            if name == 'Bx': wait += [('By', 3)]
            if name in ('Bf', 'Cy'): wait = [(n + 'x', 0)]
            if name == 'Cf': wait = [('Cy', 0)]
            here = {'Bx': (ox,), 'Bf': (x,), 'Cx': (ox,), 'Cy': (x, oy), 'Cf': (x, y)}.get(name)
            if here:
                refs, far = [R(zk, LAST).at[here]], [R(zk, CROSS).at[here]]
                if n == 'B': refs += [R('By', 3).at[here]]
                if name == 'Bf': refs += [R('Bx', 0)]
                if name == 'Cy': refs += [R('Cx', 0).at[oy]]
                if name == 'Cf': refs += [R('Cx', 0).at[y], R('Cy', 0)]
        arrive(*wait, *(farwait if middle else []))
        last = axis == 'f'
        if last: dst = fin.at[p, PART[n]]
        else:
            @pl.when(p > 0)
            def _(): send(name, p, middle).wait_send()
            dst = snd[cl].at[i]
        add(dst, [own[cl].at[i], par[cl].at[i]] + refs + (far if middle else []), lead, last)
        if not last: send(name, p, middle).start()

    def swap0(name):
        cl, i = CLASS_OF[name]
        return remote(cut(0, 0, block(name), oc), par[cl].at[i], first_s[cl].at[i], par_s[cl].at[i], NC)

    def swap(p):
        parts = [(ox, ALL, ALL, PART['A']), (ALL, ALL, ALL, PART['B']), (ALL, ALL, ALL, PART['C']), (x, ALL, ALL, PART['A'])]
        return [remote(cut(p // L, p % L, q, oc), PARTNER.at[(p, *q)], d2d_ss.at[p, i], d2d_rs.at[p, i], NC) for i, q in enumerate(parts)]

    met = greet((NX, NY, NC, dev(x, y, inner, c)), mid, dev(x, y, end, c))
    acc[...] = jnp.zeros_like(acc)
    for n in CLASS_OF: reload(n, jnp.int32(0))
    def others(f):
        def one(i):
            @pl.when(i != me)
            def _(): f((0, i))
        over(N, one)
    met()
    def both(f):
        for middle, order in enumerate(orders):
            @pl.when(mid if middle else jnp.logical_not(mid))
            def _(): f(order, middle)
    def swaps0(order, middle):
        for n, _ in sorted(order, key=lambda t: t[1]): swap0(n).start()
    both(swaps0)
    for p in range(1, NP):
        for cp in swap(p): cp.start()

    def rows(p): return remote(fin.at[p, pl.ds(Z * oc, OWN)], Ggu.at[p // L, p % L, :, c], gx_ss.at[p], gx_rs.at[p], NC)
    early = [copy(moments[k + 3 * i], MOM.at[k, i, pl.ds(Z * c, BLOCK)], mom_s.at[k, i]) for k in range(2) for i in range(2)]
    early += [copy(moments[2 + 3 * i], DOWN.at[i], mom_s.at[2, i]) for i in range(2)]
    early += [copy((wg, wu)[k].at[:, x, y, z, pl.ds(Z * c, OWN)], WGU.at[k], mom_s.at[3, k]) for k in range(2)]
    def part_of(name): return {'B': 1, 'C': 2}.get(name[0], 0 if name[1] == 'x' else 3)
    def round_(r, order, middle):
        heads = {}
        for lag in range(3):
            for n, own_lag in order:
                if own_lag == lag: heads.setdefault(part_of(n), n)
        for i, (n, lag) in enumerate(order):
            m, ml = order[(i + AHEAD) % len(order)]
            q = r + (i + AHEAD) // len(order) - ml
            @pl.when((q > 0) & (q < NP))
            def _():
                if heads[part_of(m)] == m:
                    for k in range(1, NP):
                        @pl.when(q == k)
                        def _(): swap(k)[part_of(m)].wait_recv()
                reload(m, q)
            p = r - lag
            @pl.when((p >= 0) & (p < NP))
            def _(): task(n, p, middle)
        q = r - max(lag for n, lag in order if n[1] == 'f')
        @pl.when((q >= 0) & (q < HALF))
        def _(): rows(q).start()
    def rounds(r):
        @pl.when(r == 1)
        def _():
            for cp in early: cp.start()
        both(functools.partial(round_, r))
    over(NP + max(lag for order in orders for _, lag in order), rounds)

    sall[me] = acc[0:SUB] + acc[SUB:ROWS]
    others(lambda to: remote(sall.at[me], sall.at[me], sa_ss, sa_rs, to).start())
    for l in range(L): Gd[l] = fin[HALF + l]
    for k in range(2):
        for i in range(2):
            MOM[k, i, pl.ds(BLOCK * oc, Z)] = jnp.zeros((Z, TILES, L, LANES), F32)
    for cp in early: cp.wait()
    for p in range(HALF):
        k, l = p // L, p % L
        Ggu[k, l, :, c] = fin[p, pl.ds(Z * c, OWN)]
        rows(p).wait()
    for n in CLASS_OF:
        swap0(n).wait_send()
        if n[1] != 'f': send(n, NP - 1, 0).wait_send()
    for p in range(1, NP):
        for cp in swap(p): cp.wait_send()
    rest = sall.at[pl.ds(0, N - 1)]
    got(rest, sa_rs)
    got(rest, sa_ss)
    TOT[...] = jnp.sum(sall[...], axis=0)


def rs_call(terms, weights, moments):
    bufs = [VMEM((len(names), *shape, *T3), BF) for shape, names in CLASSES.values()]
    sems = [DMA((len(names),)) for _, names in CLASSES.values()]
    scratch = bufs * 3 + [VMEM((NP, n, *CLASSES[cl][0], *T3), BF) for n, cl in ARRIVE.values()]
    scratch += [VMEM((NP, U, *T3), BF), VMEM((ROWS, LANES), F32), VMEM((N, SUB, LANES), F32)]
    scratch += sems * 4 + [DMA((NP, n)) for n, _ in ARRIVE.values()]
    scratch += [DMA((NP, 4)), DMA((NP, 4)), DMA((HALF,)), DMA((HALF,)), DMA(()), DMA(()), DMA((4, 2))]
    views = view_gu, view_gu, view_d
    return pl.pallas_call(
        functools.partial(rs_kernel, lagged(RS_ORDER)),
        out_shape=(VMEM((2, L, OWN, CORES, *T3), BF), VMEM((L, U, *T3), BF), VMEM((SUB, LANES), F32), VMEM(MOMENTS, F32), VMEM((2, L, U, *T3), F32), VMEM((2, L, OWN, CORES, *T3), BF), HBM((NP, X, Y, Z, U, *T3), BF)),
        in_specs=[HB] * 11,
        out_specs=(VM,) * 6 + (HB,),
        scratch_shapes=scratch,
        compiler_params=pltpu.CompilerParams(collective_id=0, has_side_effects=True, vmem_limit_bytes=54_800_000),
        name="reduce_scatter",
    )(*(pinned(a, HBM) for a in (*(f(a) for f, a in zip(views * 2, (*terms, *weights[:2]))), *moments)))


def up_kernel(count, Ggu, Gd, TOT, MOM, DOWN, WGU, wd, Wgu, Wd, *refs):
    new, (mom, down, wb, wdb, ld, st, ds) = refs[:6], refs[6:]
    x, y, z, c = place()
    load = copy(wd.at[:, x, y, z, c], wdb, ld)
    load.start()
    stores = []
    def store(src, dst):
        stores.append(copy(src, dst, st.at[len(stores)]))
        stores[-1].start()
    s = jnp.sum(jnp.sum(TOT[...], axis=0, keepdims=True), axis=1, keepdims=True)
    factor = jnp.minimum(1.0, 0.5 * lax.rsqrt(s * (1.0 / count) + 1e-30))
    def adamw(w, m, v, g):
        g = g * factor
        m = 0.9 * m + 0.1 * g
        v = 0.95 * v + 0.05 * g * g
        return w - 0.02 * (m * lax.rsqrt(v + 1e-8) + 0.1 * w), m, v
    rows = pl.ds(Z * c, BLOCK)
    for k in range(2):
        flat = lambda ref, i: ref.at[k, i].reshape(OWN * SUB * RUN, LANES)
        M, V, newM, newV = flat(MOM, 0), flat(MOM, 1), flat(mom, 0), flat(mom, 1)
        def tile(l, u, ch):
            base = SUB * u * RUN + TILES * ch + l
            for j in range(U):
                g, w = Ggu[k, l, u, ch, j].astype(F32), WGU[k, l, u, ch, j].astype(F32)
                half = []
                for e in range(2):
                    at = pl.ds(base + (2 * j + e) * L, SUB, stride=RUN)
                    h = slice(SUB * e, SUB * e + SUB)
                    wn, newM[at, :], newV[at, :] = adamw(w[h], M[at, :], V[at, :], g[h])
                    half.append(wn)
                wb[k, l, u, ch, j] = jnp.concatenate(half).astype(BF)
        over(L, lambda l: over(OWN, lambda u: over(CORES, lambda ch: tile(l, u, ch))))
        store(wb.at[k], Wgu.at[pl.ds(L * k, L)])
        for i in range(2): store(mom.at[k, i, rows], new[k + 3 * i])
    load.wait()
    def layer(l):
        def unit(u):
            for j in range(U):
                at = (l, u, j)
                w, m, v = adamw(wdb[at].astype(F32), DOWN[(0, *at)], DOWN[(1, *at)], Gd[at].astype(F32))
                wdb[at] = w.astype(BF)
                down[(0, *at)], down[(1, *at)] = m, v
        over(U, unit)
        for i in range(2): copy(down.at[i, l], new[2 + 3 * i].at[l], ds.at[i, l]).start()
    over(L, layer)
    store(wdb, Wd)
    for cp in stores: cp.wait()
    for l in range(L):
        for i in range(2): copy(down.at[i, l], new[2 + 3 * i].at[l], ds.at[i, l]).wait()


def view_m(m): return m.reshape(L, BLOCK, TILES, LANES).transpose(1, 2, 0, 3)
def unview_m(m): return m.transpose(2, 0, 1, 3).reshape(L, BLOCK, TILES * LANES)
def view_md(m): return tiled(m).reshape(L, U, *T3)


def up_call(sums, weights, moments):
    count = sum(w.size for w in weights)
    W, Wd = (HALF, OWN, CORES, *T3), (L, U, *T3)
    res = pl.pallas_call(
        functools.partial(up_kernel, count),
        out_shape=(HBM(W, BF), HBM(Wd, BF), *(HBM(a.shape, F32) for a in moments)),
        in_specs=[VM] * 6 + [HB],
        out_specs=[HB] * 8,
        scratch_shapes=[VMEM(MOMENTS, F32), VMEM((2, *Wd), F32), VMEM((2, L, *W[1:]), BF), VMEM(Wd, BF), DMA(()), DMA((7,)), DMA((2, L))],
        compiler_params=pltpu.CompilerParams(vmem_limit_bytes=20 * 2**20),
        name="update",
    )(*(pinned(a, VMEM) for a in sums), pinned(view_d(weights[2]), HBM))
    rows, columns = weights[2].shape[1:]
    unview = (unview_m, unview_m, lambda a: untiled(a, rows // N, columns))
    new = [f(a) for a, f in zip(res[2:], unview * 2)]
    return res[0], res[1], new


AG_ORDER = [
    ['Bo', 'Co', 'Ax0_0++', 'Ao', 'Cx+', 'By_0++', 'Az_2+', 'Ay_1+', 'Ax0_3++', 'Bz_3++', 'By_1++', 'Bz_1+', 'Cy', 'Ax1_1++', 'Ay_3++', 'Cz_2++', 'Ax0_2++', 'Cz_1++', 'Az_3+', 'Bx', 'By_2++', 'Bz_2+', 'Ay_2+', 'Ax1_2++', 'Ax1_0+', 'Ax0_1+', 'Ay_0', 'Ax1_3++', 'Az_1', 'Cz_3++', 'By_3++'],
    ['Co', 'Bo+', 'Bz_3++', 'Ao', 'Az_2+', 'Az_1+', 'Ay_2++', 'Cx++', 'Ax0_0+', 'Cz_2++', 'Bx+', 'Ay_3++', 'Ax0_3++', 'Az_3+', 'Cz_3++', 'By_2++', 'Cy+', 'Bz_1+', 'Ax1_1++', 'Ay_1+', 'By_0++', 'Bz_2+', 'Ay_0+', 'Ax0_2++', 'By_1++', 'Ax1_0++', 'Ax0_1++', 'Ax1_2++', 'Ax1_3++', 'Cz_1+', 'By_3++'],
]


def ag_kernel(orders, wgu, wd, VO, tmp, own_s, ex_ss, ex_rs, xs, ys, zis, zos, ds, dr, axr, ayr, azr, byr, bzr, bxr, czr, cxr, cyr):
    x, y, z, c = place()
    ox, oy, oc = 1 - x, 1 - y, 1 - c
    mid, sl, inner, end = line(z)
    NX, NY, NC, ZI, ZO = dev(ox, y, z, c), dev(x, oy, z, c), dev(x, y, z, oc), dev(x, y, inner, c), dev(x, y, end, c)
    zr = {'A': azr, 'B': bzr, 'C': czr}

    def task(name, p, middle):
        n, axis, i = split(name)
        zz = sl[i]
        def at(idx): return VO.at[(p, *idx, PART[n], c)]
        def push(idx, to, ss, rs): remote(at(idx), at(idx), ss.at[p], rs, to).start()
        def give(idx): push(idx, NC, ds, dr.at[p])
        def chain(idx):
            rs = zr[n].at[p, zz]
            if i == 0 or middle and i == 1: push(idx, ZI, zis, rs)
            if middle and i != 1: push(idx, ZO, zos, rs)
        if axis == 'o':
            here = x, y, z
            if n == 'A':
                chain(here)
                push(here, NY, ys, ayr.at[p, z])
                push(here, NX, xs, axr.at[p, z, 0])
            elif n == 'B': push(here, NX, xs, bxr.at[p])
            else: push(here, NY, ys, cyr.at[p])
            give(here)
        elif n == 'A':
            if axis == 'z':
                here = x, y, zz
                got(at(here), azr.at[p, zz])
                chain(here)
                push(here, NY, ys, ayr.at[p, zz])
                push(here, NX, xs, axr.at[p, zz, 0])
            elif axis == 'y':
                here = x, oy, zz
                got(at(here), ayr.at[p, zz])
                push(here, NX, xs, axr.at[p, zz, 1])
            else:
                k = int(name[2])
                here = ox, (oy if k else y), zz
                got(at(here), axr.at[p, zz, k])
            give(here)
        elif n == 'B':
            here, wide = (ox, y, z), (ALL, y, zz)
            if axis == 'y':
                here = ALL, oy, zz
                got(at(here), byr.at[p, zz])
            else:
                if axis == 'x': got(at(here), bxr.at[p])
                else:
                    here = wide
                    got(at(here), bzr.at[p, zz])
                chain(wide)
                push(wide, NY, ys, byr.at[p, zz])
            give(here)
        elif axis == 'y':
            here = x, oy, z
            got(at(here), cyr.at[p])
            push((x, ALL, z), NX, xs, cxr.at[p])
            give(here)
        else:
            here, wide = (ox, ALL, z), (ALL, ALL, zz)
            if axis == 'x': got(at(here), cxr.at[p])
            else:
                here = wide
                got(at(here), czr.at[p, zz])
            chain(wide)
            give(here)

    met = greet((NX, NY, NC, ZI), mid, ZO)
    mine = VO.at[:, x, y, z]
    own = [copy(wd.at[l], mine.at[l, :, c], own_s.at[l]) for l in range(L)]
    own += [copy(wgu.at[q, pl.ds(c, Z), c], mine.at[L + q, pl.ds(OWN * c, Z), c], own_s.at[L + q]) for q in range(HALF)]
    own += [copy(wgu.at[:, Z * oc, c], tmp.at[0], own_s.at[NP])]
    for cp in own: cp.start()
    met()
    swap = [remote(wgu.at[q, pl.ds(c, Z), oc], mine.at[L + q, pl.ds(OWN * c, Z), oc], ex_ss.at[q], ex_rs.at[q], NC) for q in range(HALF)]
    swap += [remote(wgu.at[:, Z * oc, oc], tmp.at[1], ex_ss.at[HALF], ex_rs.at[HALF], NC)]
    for cp in swap: cp.start()
    for cp in own[:L]: cp.wait()

    def round_(r):
        @pl.when(r == 1)
        def _():
            for cp in own[L:] + swap: cp.wait()
            upper = lax.broadcasted_iota(jnp.int32, T3, 1) % SUB < Z
            first = upper.astype(jnp.int32) == oc
            for q in range(HALF):
                VO[L + q, x, y, z, Z, c] = jnp.where(first, tmp[0, q].astype(F32), tmp[1, q].astype(F32)).astype(BF)
        for middle, order in enumerate(orders):
            @pl.when(mid if middle else jnp.logical_not(mid))
            def _():
                for n, lag in order:
                    p = r - lag
                    @pl.when((p >= 0) & (p < NP))
                    def _(): task(n, p, middle)
    over(NP + max(lag for order in orders for _, lag in order), round_)

    def finish(p):
        q = VO.at[pl.ds(0, 5), 0, 0, 0, :, 0]
        got(q, xs.at[p])
        got(q, ys.at[p])
        @pl.when(mid)
        def _():
            got(q.at[:, pl.ds(0, 6)], zis.at[p])
            got(q, zos.at[p])
        @pl.when(jnp.logical_not(mid))
        def _(): got(q.at[:, pl.ds(0, 3)], zis.at[p])
        whole = VO.at[0, :, :, :, :, 0]
        got(whole, ds.at[p])
        got(whole, dr.at[p])
    over(NP, finish)


def place_kernel(VO, og, ou, od, sems):
    out = []
    def put(src, dst):
        out.append(copy(src, dst, sems.at[len(out)]))
        out[-1].start()
    for l in range(L):
        for i in range(X):
            for k in range(CORES): put(VO.at[l, i, :, :, :, k], od.at[l, i, :, :, k])
            put(VO.at[L + l, i], og.at[l, i])
            put(VO.at[2 * L + l, i], ou.at[l, i])
    for cp in out: cp.wait()


def ag_call(wgu, wd):
    four = DMA((NP, Z))
    one = DMA((NP,))
    VO = pl.pallas_call(
        functools.partial(ag_kernel, lagged(AG_ORDER)),
        out_shape=VMEM((NP, X, Y, Z, U, CORES, *T3), BF),
        in_specs=[HB] * 2,
        out_specs=VM,
        scratch_shapes=[VMEM((2, HALF, *T3), BF), DMA((NP + 1,)), DMA((HALF + 1,)), DMA((HALF + 1,))] + [one] * 6 + [DMA((NP, Z, 2)), four, four, four, four, one, four, one, one],
        compiler_params=pltpu.CompilerParams(collective_id=1, has_side_effects=True, vmem_limit_bytes=2**20),
        name="all_gather",
    )(pinned(wgu, HBM), pinned(wd, HBM))
    G = jax.ShapeDtypeStruct((L, X, Y, Z, U, CORES, *T3), BF)
    D = jax.ShapeDtypeStruct((L, X, Y, Z, CORES, U, *T3), BF)
    og, ou, od = pl.pallas_call(
        place_kernel, out_shape=(G, G, D), in_specs=[VM], out_specs=(ANY,) * 3, scratch_shapes=[DMA((16,))],
        compiler_params=pltpu.CompilerParams(vmem_limit_bytes=2**20), name="place",
    )(pinned(VO, VMEM))
    return og, ou, od


def solution(mesh):
    def step(*arrays):
        terms, weights, m, v = (arrays[i : i + 3] for i in range(0, 12, 3))
        moments = [f(a) for a, f in zip((*m, *v), (view_m, view_m, view_md) * 2)]
        *sums, _ = rs_call([t[0] for t in terms], weights, moments)
        Wgu, Wd, new = up_call(sums, weights, moments)
        whole = [untiled(a, *w.shape[1:]) for a, w in zip(ag_call(Wgu, Wd), weights)]
        return (*whole, *new)

    all_of, cut = P(None, None, None), P(None, "dp", None)
    return jax.shard_map(
        step,
        mesh=mesh,
        in_specs=(P(("rep", "dp"), None, None, None),) * 3 + (all_of,) * 3 + (cut,) * 6,
        out_specs=(P("rep", None, None),) * 3 + (P("rep", "dp", None),) * 6,
        check_vma=False,
    )
```

```python
import functools

import jax
import jax.numpy as jnp
from jax import lax
from jax.experimental import pallas as pl
from jax.experimental.pallas import tpu as pltpu
from jax.sharding import PartitionSpec as P

MESH = pl.DeviceIdType.MESH
BF, F32 = jnp.bfloat16, jnp.float32
DMA = pltpu.SemaphoreType.DMA
VMEM, HBM = pltpu.VMEM, pltpu.HBM
ALL = slice(None)
L, X, Y, Z, U, CORES = 2, 2, 2, 4, 9, 2
N = X * Y * Z * CORES
SUB, ROWS, LANES = 8, 16, 128
T3 = (U, ROWS, LANES)
NP = 3 * L
HALF = NP - L
OWN = 5
PART = {'A': pl.ds(0, OWN), 'B': pl.ds(OWN, 3), 'C': U - 1}
BLOCK, TILES = 36, 36
RUN = TILES * L
MOMENTS = (2, 2, OWN * SUB, TILES, L, LANES)
VM, HB, ANY = (pl.BlockSpec(memory_space=s) for s in (VMEM, HBM, pl.ANY))


def tiled(a):
    l, r, c = a.shape
    return a.reshape(l, r // SUB, SUB, c // LANES, LANES).swapaxes(2, 3)


def untiled(a, r, c):
    return a.reshape(L, r // SUB, c // LANES, SUB, LANES).swapaxes(2, 3).reshape(L, r, c)


def view_gu(g): return tiled(g).reshape(L, X, Y, Z, U, CORES, *T3)
def view_d(g): return tiled(g).reshape(L, X, Y, Z, CORES, U, *T3)


def place():
    d = lax.axis_index("dp")
    d, c = d // CORES, d % CORES
    d, z = d // Z, d % Z
    return d // Y, d % Y, z, c


def dev(x, y, z, c): return 0, ((x * Y + y) * Z + z) * CORES + c


def line(z):
    h = z // 2
    return (z == 1) | (z == 2), [z, 1 - z + Z * h, 2 - h, 3 - 3 * h], z + 1 - 2 * h, 3 * h


def over(n, f): lax.fori_loop(0, n, lambda i, _: (f(i), 0)[1], 0)


def copy(src, dst, sem): return pltpu.make_async_copy(src, dst, sem)


def remote(src, dst, ss, rs, to): return pltpu.make_async_remote_copy(src, dst, ss, rs, device_id=to, device_id_type=MESH)


def got(ref, sem): copy(ref, ref, sem).wait()


def greet(to, mid, too):
    barrier = pltpu.get_barrier_semaphore()
    def signal(one): pl.semaphore_signal(barrier, 1, device_id=one, device_id_type=MESH)
    for one in to: signal(one)
    @pl.when(mid)
    def _(): signal(too)
    return lambda: pl.semaphore_wait(barrier, len(to) + mid.astype(jnp.int32))


def pinned(a, space): return pltpu.with_memory_space_constraint(a, space)


def split(name): return name[0], name[1], int(name[-1]) if name[-1].isdigit() else 0


def lagged(orders): return [[(n.rstrip('+'), n.count('+')) for n in names] for names in orders]


RS_ORDER = [
    ['Cz0', 'By0', 'Ax0', 'Cz2', 'Az0+', 'By1', 'Cz1', 'Ay1+', 'Ax4', 'Ax5', 'Ay3++', 'Az2++', 'By2', 'Bz0', 'Cy++', 'Ay2+', 'Az1+', 'Ax1', 'Ay0', 'Bx++', 'Ax2', 'By3+', 'Ax6+', 'Cx+', 'Ax7+', 'Af++', 'Bz1', 'Bz2+', 'Cf++', 'Ax3', 'Bf++'],
    ['Cz1+', 'Cz2+', 'By1', 'Ax0', 'Ax1', 'Ay2+', 'Ax7++', 'Az1++', 'By0', 'Ax2', 'Ay0', 'Bz1+', 'Az2++', 'Cz0', 'Cy++', 'Ax4', 'Ax3', 'Bx++', 'By3+', 'Ax6+', 'By2', 'Bz2+', 'Az0+', 'Ax5', 'Ay1', 'Ay3+', 'Cx+', 'Bz0', 'Af++', 'Cf++', 'Bf++'],
]
AHEAD = 5
CLASSES = {
    'A': ((OWN,), ['Ax0', 'Ax1', 'Ax2', 'Ax3', 'Ax4', 'Ax5', 'Ax6', 'Ax7', 'Ay0', 'Ay1', 'Ay2', 'Ay3', 'Az0', 'Az1', 'Az2', 'Af']),
    'By': ((X, 3), ['By0', 'By1', 'By2', 'By3', 'Bz0', 'Bz1', 'Bz2']),
    'Bx': ((3,), ['Bx', 'Bf']),
    'Cz': ((X, Y), ['Cz0', 'Cz1', 'Cz2']),
    'Cx': ((Y,), ['Cx']),
    'Cy': ((), ['Cy', 'Cf']),
}
CLASS_OF = {n: (k, i) for k, (_, names) in CLASSES.items() for i, n in enumerate(names)}
ARRIVE = {'Ax': (8, 'A'), 'Ay': (Z, 'A'), 'Az': (5, 'A'), 'By': (Z, 'By'), 'Bz': (5, 'By'), 'Bx': (1, 'Bx'), 'Cz': (5, 'Cz'), 'Cx': (1, 'Cx'), 'Cy': (1, 'Cy')}
LAST, CROSS = 2, 4


def rs_kernel(orders, gg, gu, gd, wg, wu, *refs):
    moments, (Ggu, Gd, TOT, MOM, DOWN, WGU, PARTNER), scr = refs[:6], refs[6:13], iter(refs[13:])
    take = lambda names: {n: next(scr) for n in names}
    own, par, snd, rcv = take(CLASSES), take(CLASSES), take(CLASSES), take(ARRIVE)
    fin, acc, sall = take(range(3)).values()
    own_s, par_s, snd_s, first_s, rcv_s = take(CLASSES), take(CLASSES), take(CLASSES), take(CLASSES), take(ARRIVE)
    d2d_ss, d2d_rs, gx_ss, gx_rs, sa_ss, sa_rs, mom_s = take(range(7)).values()
    x, y, z, c = place()
    ox, oy, oc = 1 - x, 1 - y, 1 - c
    me = lax.axis_index("dp")
    mid, near, inner, end = line(z)
    zo = near[::-1]
    side = z + 1 - 2 * (z % 2)
    NX, NY, NC = dev(ox, y, z, c), dev(x, oy, z, c), dev(x, y, z, oc)

    def block(name):
        n, axis, i = split(name)
        u = PART[n]
        if axis == 'f': return x, y, z, u
        if n == 'A':
            if axis == 'x': return ox, (oy if i < Z else y), zo[i % Z], u
            return x, (oy if axis == 'y' else y), zo[i], u
        if n == 'B':
            if axis == 'x': return ox, y, z, u
            return ALL, (oy if axis == 'y' else y), zo[i], u
        return {'z': (ALL, ALL, zo[i], u), 'x': (ox, ALL, z, u), 'y': (x, oy, z, u)}[axis]

    def cut(k, l, b, core):
        return gd.at[(l, *b[:3], core, b[3])] if k == 2 else (gg, gu)[k].at[(l, *b, core)]

    def reload(name, p):
        cl, i = CLASS_OF[name]
        b = block(name)
        @pl.when((p >= 0) & (p < NP))
        def _():
            for k in range(3):
                @pl.when(p // L == k)
                def _(): copy(cut(k, p % L, b, c), own[cl].at[i], own_s[cl].at[i]).start()
            @pl.when(p > 0)
            def _(): copy(PARTNER.at[(p, *b)], par[cl].at[i], par_s[cl].at[i]).start()

    def send(name, p, middle):
        cl, i = CLASS_OF[name]
        n, axis, j = split(name)
        if axis == 'x': to, slot = NX, j
        elif axis == 'y': to, slot = NY, j
        elif j < 2: to, slot = dev(x, y, inner, c), j + 3 * middle
        else: to, slot = dev(x, y, side, c), LAST
        kind = name[:2]
        return remote(snd[cl].at[i], rcv[kind].at[p, slot], snd_s[cl].at[i], rcv_s[kind].at[p, slot], to)

    def add(dst, refs, lead, last):
        def one(*idx):
            at = idx if idx else ...
            t = sum(r[at].astype(F32) for r in refs).astype(BF)
            dst[at] = t
            if last:
                t = t.astype(F32)
                acc[...] += jnp.sum(t * t, axis=0)
        if not lead: one()
        elif len(lead) == 1: over(lead[0], one)
        else: over(lead[0], lambda i: over(lead[1], lambda j: one(i, j)))

    def task(name, p, middle):
        cl, i = CLASS_OF[name]
        n, axis, j = split(name)
        lead = CLASSES[cl][0]
        R = lambda kind, s: rcv[kind].at[p, s]
        def arrive(*which):
            for kind, s in which: got(R(kind, s), rcv_s[kind].at[p, s])
        got(own[cl].at[i], own_s[cl].at[i])
        got(par[cl].at[i], par_s[cl].at[i])
        zk, refs, far, wait, farwait = n + 'z', [], [], [], []
        if axis == 'z':
            s = (0, 1, 3)[j]
            far, farwait = [R(zk, s)], [(zk, s)]
            wait = {'A': [('Ax', Z + j), ('Ay', j)], 'B': [('By', j)], 'C': []}[n]
            refs = [R(*w) for w in wait]
        elif name[:2] == 'Ay':
            wait = [('Ax', j)]
            refs = [R(*w) for w in wait]
        elif name == 'Af':
            wait, farwait = [('Ax', Z + 3), ('Ay', 3), (zk, LAST)], [(zk, CROSS)]
            refs, far = [R(*w) for w in wait], [R(zk, CROSS)]
        elif axis != 'y' or n == 'C':
            if n == 'B' and axis == 'x' or n == 'C' and axis == 'x': wait, farwait = [(zk, LAST)], [(zk, CROSS)]
            if name == 'Bx': wait += [('By', 3)]
            if name in ('Bf', 'Cy'): wait = [(n + 'x', 0)]
            if name == 'Cf': wait = [('Cy', 0)]
            here = {'Bx': (ox,), 'Bf': (x,), 'Cx': (ox,), 'Cy': (x, oy), 'Cf': (x, y)}.get(name)
            if here:
                refs, far = [R(zk, LAST).at[here]], [R(zk, CROSS).at[here]]
                if n == 'B': refs += [R('By', 3).at[here]]
                if name == 'Bf': refs += [R('Bx', 0)]
                if name == 'Cy': refs += [R('Cx', 0).at[oy]]
                if name == 'Cf': refs += [R('Cx', 0).at[y], R('Cy', 0)]
        arrive(*wait, *(farwait if middle else []))
        last = axis == 'f'
        if last: dst = fin.at[p, PART[n]]
        else:
            @pl.when(p > 0)
            def _(): send(name, p, middle).wait_send()
            dst = snd[cl].at[i]
        add(dst, [own[cl].at[i], par[cl].at[i]] + refs + (far if middle else []), lead, last)
        if not last: send(name, p, middle).start()

    def swap0(name):
        cl, i = CLASS_OF[name]
        return remote(cut(0, 0, block(name), oc), par[cl].at[i], first_s[cl].at[i], par_s[cl].at[i], NC)

    def swap(p):
        parts = [(ox, ALL, ALL, PART['A']), (ALL, ALL, ALL, PART['B']), (ALL, ALL, ALL, PART['C']), (x, ALL, ALL, PART['A'])]
        return [remote(cut(p // L, p % L, q, oc), PARTNER.at[(p, *q)], d2d_ss.at[p, i], d2d_rs.at[p, i], NC) for i, q in enumerate(parts)]

    met = greet((NX, NY, NC, dev(x, y, inner, c)), mid, dev(x, y, end, c))
    acc[...] = jnp.zeros_like(acc)
    for n in CLASS_OF: reload(n, jnp.int32(0))
    def others(f):
        def one(i):
            @pl.when(i != me)
            def _(): f((0, i))
        over(N, one)
    met()
    def both(f):
        for middle, order in enumerate(orders):
            @pl.when(mid if middle else jnp.logical_not(mid))
            def _(): f(order, middle)
    def swaps0(order, middle):
        for n, _ in sorted(order, key=lambda t: t[1]): swap0(n).start()
    both(swaps0)
    for p in range(1, NP):
        for cp in swap(p): cp.start()

    def rows(p): return remote(fin.at[p, pl.ds(Z * oc, OWN)], Ggu.at[p // L, p % L, :, c], gx_ss.at[p], gx_rs.at[p], NC)
    early = [copy(moments[k + 3 * i], MOM.at[k, i, pl.ds(Z * c, BLOCK)], mom_s.at[k, i]) for k in range(2) for i in range(2)]
    early += [copy(moments[2 + 3 * i], DOWN.at[i], mom_s.at[2, i]) for i in range(2)]
    early += [copy((wg, wu)[k].at[:, x, y, z, pl.ds(Z * c, OWN)], WGU.at[k], mom_s.at[3, k]) for k in range(2)]
    def part_of(name): return {'B': 1, 'C': 2}.get(name[0], 0 if name[1] == 'x' else 3)
    def round_(r, order, middle):
        heads = {}
        for lag in range(3):
            for n, own_lag in order:
                if own_lag == lag: heads.setdefault(part_of(n), n)
        for i, (n, lag) in enumerate(order):
            m, ml = order[(i + AHEAD) % len(order)]
            q = r + (i + AHEAD) // len(order) - ml
            @pl.when((q > 0) & (q < NP))
            def _():
                if heads[part_of(m)] == m:
                    for k in range(1, NP):
                        @pl.when(q == k)
                        def _(): swap(k)[part_of(m)].wait_recv()
                reload(m, q)
            p = r - lag
            @pl.when((p >= 0) & (p < NP))
            def _(): task(n, p, middle)
        q = r - max(lag for n, lag in order if n[1] == 'f')
        @pl.when((q >= 0) & (q < HALF))
        def _(): rows(q).start()
    def rounds(r):
        @pl.when(r == 1)
        def _():
            for cp in early: cp.start()
        both(functools.partial(round_, r))
    over(NP + max(lag for order in orders for _, lag in order), rounds)

    sall[me] = acc[0:SUB] + acc[SUB:ROWS]
    others(lambda to: remote(sall.at[me], sall.at[me], sa_ss, sa_rs, to).start())
    for l in range(L): Gd[l] = fin[HALF + l]
    for k in range(2):
        for i in range(2):
            MOM[k, i, pl.ds(BLOCK * oc, Z)] = jnp.zeros((Z, TILES, L, LANES), F32)
    for cp in early: cp.wait()
    for p in range(HALF):
        k, l = p // L, p % L
        Ggu[k, l, :, c] = fin[p, pl.ds(Z * c, OWN)]
        rows(p).wait()
    for n in CLASS_OF:
        swap0(n).wait_send()
        if n[1] != 'f': send(n, NP - 1, 0).wait_send()
    for p in range(1, NP):
        for cp in swap(p): cp.wait_send()
    rest = sall.at[pl.ds(0, N - 1)]
    got(rest, sa_rs)
    got(rest, sa_ss)
    TOT[...] = jnp.sum(sall[...], axis=0)


def rs_call(terms, weights, moments):
    bufs = [VMEM((len(names), *shape, *T3), BF) for shape, names in CLASSES.values()]
    sems = [DMA((len(names),)) for _, names in CLASSES.values()]
    scratch = bufs * 3 + [VMEM((NP, n, *CLASSES[cl][0], *T3), BF) for n, cl in ARRIVE.values()]
    scratch += [VMEM((NP, U, *T3), BF), VMEM((ROWS, LANES), F32), VMEM((N, SUB, LANES), F32)]
    scratch += sems * 4 + [DMA((NP, n)) for n, _ in ARRIVE.values()]
    scratch += [DMA((NP, 4)), DMA((NP, 4)), DMA((HALF,)), DMA((HALF,)), DMA(()), DMA(()), DMA((4, 2))]
    views = view_gu, view_gu, view_d
    return pl.pallas_call(
        functools.partial(rs_kernel, lagged(RS_ORDER)),
        out_shape=(VMEM((2, L, OWN, CORES, *T3), BF), VMEM((L, U, *T3), BF), VMEM((SUB, LANES), F32), VMEM(MOMENTS, F32), VMEM((2, L, U, *T3), F32), VMEM((2, L, OWN, CORES, *T3), BF), HBM((NP, X, Y, Z, U, *T3), BF)),
        in_specs=[HB] * 11,
        out_specs=(VM,) * 6 + (HB,),
        scratch_shapes=scratch,
        compiler_params=pltpu.CompilerParams(collective_id=0, has_side_effects=True, vmem_limit_bytes=54_800_000),
        name="reduce_scatter",
    )(*(pinned(a, HBM) for a in (*(f(a) for f, a in zip(views * 2, (*terms, *weights[:2]))), *moments)))


def up_kernel(count, Ggu, Gd, TOT, MOM, DOWN, WGU, wd, Wgu, Wd, *refs):
    new, (mom, down, wb, wdb, ld, st, ds) = refs[:6], refs[6:]
    x, y, z, c = place()
    load = copy(wd.at[:, x, y, z, c], wdb, ld)
    load.start()
    stores = []
    def store(src, dst):
        stores.append(copy(src, dst, st.at[len(stores)]))
        stores[-1].start()
    s = jnp.sum(jnp.sum(TOT[...], axis=0, keepdims=True), axis=1, keepdims=True)
    factor = jnp.minimum(1.0, 0.5 * lax.rsqrt(s * (1.0 / count) + 1e-30))
    def adamw(w, m, v, g):
        g = g * factor
        m = 0.9 * m + 0.1 * g
        v = 0.95 * v + 0.05 * g * g
        return w - 0.02 * (m * lax.rsqrt(v + 1e-8) + 0.1 * w), m, v
    for k in range(2):
        flat = lambda ref, i: ref.at[k, i].reshape(OWN * SUB * RUN, LANES)
        M, V, newM, newV = flat(MOM, 0), flat(MOM, 1), flat(mom, 0), flat(mom, 1)
        def tile(l, u, ch):
            base = SUB * u * RUN + TILES * ch + l
            for j in range(U):
                g, w = Ggu[k, l, u, ch, j].astype(F32), WGU[k, l, u, ch, j].astype(F32)
                half = []
                for e in range(2):
                    at = pl.ds(base + (2 * j + e) * L, SUB, stride=RUN)
                    h = slice(SUB * e, SUB * e + SUB)
                    wn, newM[at, :], newV[at, :] = adamw(w[h], M[at, :], V[at, :], g[h])
                    half.append(wn)
                wb[k, l, u, ch, j] = jnp.concatenate(half).astype(BF)
        for tiles, (row, n) in zip((range(3), range(3, OWN)), ((0, ROWS), (ROWS, BLOCK - ROWS))):
            def both(u):
                over(L, lambda l: [tile(l, tiles[0] + u, ch) for ch in range(CORES)])
            over(len(tiles), both)
            for i in range(2): store(mom.at[k, i, pl.ds(Z * c + row, n)], new[k + 3 * i].at[pl.ds(row, n)])
        store(wb.at[k], Wgu.at[pl.ds(L * k, L)])
    load.wait()
    def layer(l):
        def unit(u):
            for j in range(U):
                at = (l, u, j)
                w, m, v = adamw(wdb[at].astype(F32), DOWN[(0, *at)], DOWN[(1, *at)], Gd[at].astype(F32))
                wdb[at] = w.astype(BF)
                down[(0, *at)], down[(1, *at)] = m, v
        over(U, unit)
        for i in range(2): copy(down.at[i, l], new[2 + 3 * i].at[l], ds.at[i, l]).start()
    over(L, layer)
    store(wdb, Wd)
    for cp in stores: cp.wait()
    for l in range(L):
        for i in range(2): copy(down.at[i, l], new[2 + 3 * i].at[l], ds.at[i, l]).wait()


def view_m(m): return m.reshape(L, BLOCK, TILES, LANES).transpose(1, 2, 0, 3)
def unview_m(m): return m.transpose(2, 0, 1, 3).reshape(L, BLOCK, TILES * LANES)
def view_md(m): return tiled(m).reshape(L, U, *T3)


def up_call(sums, weights, moments):
    count = sum(w.size for w in weights)
    W, Wd = (HALF, OWN, CORES, *T3), (L, U, *T3)
    res = pl.pallas_call(
        functools.partial(up_kernel, count),
        out_shape=(HBM(W, BF), HBM(Wd, BF), *(HBM(a.shape, F32) for a in moments)),
        in_specs=[VM] * 6 + [HB],
        out_specs=[HB] * 8,
        scratch_shapes=[VMEM(MOMENTS, F32), VMEM((2, *Wd), F32), VMEM((2, L, *W[1:]), BF), VMEM(Wd, BF), DMA(()), DMA((11,)), DMA((2, L))],
        compiler_params=pltpu.CompilerParams(vmem_limit_bytes=20 * 2**20),
        name="update",
    )(*(pinned(a, VMEM) for a in sums), pinned(view_d(weights[2]), HBM))
    rows, columns = weights[2].shape[1:]
    unview = (unview_m, unview_m, lambda a: untiled(a, rows // N, columns))
    new = [f(a) for a, f in zip(res[2:], unview * 2)]
    return res[0], res[1], new


AG_ORDER = [
    ['Bo', 'Co', 'Ax0_0++', 'Ao', 'Cx+', 'By_0++', 'Az_2+', 'Ay_1+', 'Ax0_3++', 'Bz_3++', 'By_1++', 'Bz_1+', 'Cy', 'Ax1_1++', 'Ay_3++', 'Cz_2++', 'Ax0_2++', 'Cz_1++', 'Az_3+', 'Bx', 'By_2++', 'Bz_2+', 'Ay_2+', 'Ax1_2++', 'Ax1_0+', 'Ax0_1+', 'Ay_0', 'Ax1_3++', 'Az_1', 'Cz_3++', 'By_3++'],
    ['Co', 'Bo+', 'Bz_3++', 'Ao', 'Az_2+', 'Az_1+', 'Ay_2++', 'Cx++', 'Ax0_0+', 'Cz_2++', 'Bx+', 'Ay_3++', 'Ax0_3++', 'Az_3+', 'Cz_3++', 'By_2++', 'Cy+', 'Bz_1+', 'Ax1_1++', 'Ay_1+', 'By_0++', 'Bz_2+', 'Ay_0+', 'Ax0_2++', 'By_1++', 'Ax1_0++', 'Ax0_1++', 'Ax1_2++', 'Ax1_3++', 'Cz_1+', 'By_3++'],
]


def ag_kernel(orders, wgu, wd, VO, tmp, own_s, ex_ss, ex_rs, xs, ys, zis, zos, ds, dr, axr, ayr, azr, byr, bzr, bxr, czr, cxr, cyr):
    x, y, z, c = place()
    ox, oy, oc = 1 - x, 1 - y, 1 - c
    mid, sl, inner, end = line(z)
    NX, NY, NC, ZI, ZO = dev(ox, y, z, c), dev(x, oy, z, c), dev(x, y, z, oc), dev(x, y, inner, c), dev(x, y, end, c)
    zr = {'A': azr, 'B': bzr, 'C': czr}

    def task(name, p, middle):
        n, axis, i = split(name)
        zz = sl[i]
        def at(idx): return VO.at[(p, *idx, PART[n], c)]
        def push(idx, to, ss, rs): remote(at(idx), at(idx), ss.at[p], rs, to).start()
        def give(idx): push(idx, NC, ds, dr.at[p])
        def chain(idx):
            rs = zr[n].at[p, zz]
            if i == 0 or middle and i == 1: push(idx, ZI, zis, rs)
            if middle and i != 1: push(idx, ZO, zos, rs)
        if axis == 'o':
            here = x, y, z
            if n == 'A':
                chain(here)
                push(here, NY, ys, ayr.at[p, z])
                push(here, NX, xs, axr.at[p, z, 0])
            elif n == 'B': push(here, NX, xs, bxr.at[p])
            else: push(here, NY, ys, cyr.at[p])
            give(here)
        elif n == 'A':
            if axis == 'z':
                here = x, y, zz
                got(at(here), azr.at[p, zz])
                chain(here)
                push(here, NY, ys, ayr.at[p, zz])
                push(here, NX, xs, axr.at[p, zz, 0])
            elif axis == 'y':
                here = x, oy, zz
                got(at(here), ayr.at[p, zz])
                push(here, NX, xs, axr.at[p, zz, 1])
            else:
                k = int(name[2])
                here = ox, (oy if k else y), zz
                got(at(here), axr.at[p, zz, k])
            give(here)
        elif n == 'B':
            here, wide = (ox, y, z), (ALL, y, zz)
            if axis == 'y':
                here = ALL, oy, zz
                got(at(here), byr.at[p, zz])
            else:
                if axis == 'x': got(at(here), bxr.at[p])
                else:
                    here = wide
                    got(at(here), bzr.at[p, zz])
                chain(wide)
                push(wide, NY, ys, byr.at[p, zz])
            give(here)
        elif axis == 'y':
            here = x, oy, z
            got(at(here), cyr.at[p])
            push((x, ALL, z), NX, xs, cxr.at[p])
            give(here)
        else:
            here, wide = (ox, ALL, z), (ALL, ALL, zz)
            if axis == 'x': got(at(here), cxr.at[p])
            else:
                here = wide
                got(at(here), czr.at[p, zz])
            chain(wide)
            give(here)

    met = greet((NX, NY, NC, ZI), mid, ZO)
    mine = VO.at[:, x, y, z]
    own = [copy(wd.at[l], mine.at[l, :, c], own_s.at[l]) for l in range(L)]
    own += [copy(wgu.at[q, pl.ds(c, Z), c], mine.at[L + q, pl.ds(OWN * c, Z), c], own_s.at[L + q]) for q in range(HALF)]
    own += [copy(wgu.at[:, Z * oc, c], tmp.at[0], own_s.at[NP])]
    for cp in own: cp.start()
    met()
    swap = [remote(wgu.at[q, pl.ds(c, Z), oc], mine.at[L + q, pl.ds(OWN * c, Z), oc], ex_ss.at[q], ex_rs.at[q], NC) for q in range(HALF)]
    swap += [remote(wgu.at[:, Z * oc, oc], tmp.at[1], ex_ss.at[HALF], ex_rs.at[HALF], NC)]
    for cp in swap: cp.start()
    for cp in own[:L]: cp.wait()

    def round_(r):
        @pl.when(r == 1)
        def _():
            for cp in own[L:] + swap: cp.wait()
            upper = lax.broadcasted_iota(jnp.int32, T3, 1) % SUB < Z
            first = upper.astype(jnp.int32) == oc
            for q in range(HALF):
                VO[L + q, x, y, z, Z, c] = jnp.where(first, tmp[0, q].astype(F32), tmp[1, q].astype(F32)).astype(BF)
        for middle, order in enumerate(orders):
            @pl.when(mid if middle else jnp.logical_not(mid))
            def _():
                for n, lag in order:
                    p = r - lag
                    @pl.when((p >= 0) & (p < NP))
                    def _(): task(n, p, middle)
    over(NP + max(lag for order in orders for _, lag in order), round_)

    def finish(p):
        q = VO.at[pl.ds(0, 5), 0, 0, 0, :, 0]
        got(q, xs.at[p])
        got(q, ys.at[p])
        @pl.when(mid)
        def _():
            got(q.at[:, pl.ds(0, 6)], zis.at[p])
            got(q, zos.at[p])
        @pl.when(jnp.logical_not(mid))
        def _(): got(q.at[:, pl.ds(0, 3)], zis.at[p])
        whole = VO.at[0, :, :, :, :, 0]
        got(whole, ds.at[p])
        got(whole, dr.at[p])
    over(NP, finish)


def place_kernel(VO, og, ou, od, sems):
    out = []
    def put(src, dst):
        out.append(copy(src, dst, sems.at[len(out)]))
        out[-1].start()
    for l in range(L):
        for i in range(X):
            for k in range(CORES): put(VO.at[l, i, :, :, :, k], od.at[l, i, :, :, k])
            put(VO.at[L + l, i], og.at[l, i])
            put(VO.at[2 * L + l, i], ou.at[l, i])
    for cp in out: cp.wait()


def ag_call(wgu, wd):
    four = DMA((NP, Z))
    one = DMA((NP,))
    VO = pl.pallas_call(
        functools.partial(ag_kernel, lagged(AG_ORDER)),
        out_shape=VMEM((NP, X, Y, Z, U, CORES, *T3), BF),
        in_specs=[HB] * 2,
        out_specs=VM,
        scratch_shapes=[VMEM((2, HALF, *T3), BF), DMA((NP + 1,)), DMA((HALF + 1,)), DMA((HALF + 1,))] + [one] * 6 + [DMA((NP, Z, 2)), four, four, four, four, one, four, one, one],
        compiler_params=pltpu.CompilerParams(collective_id=1, has_side_effects=True, vmem_limit_bytes=2**20),
        name="all_gather",
    )(pinned(wgu, HBM), pinned(wd, HBM))
    G = jax.ShapeDtypeStruct((L, X, Y, Z, U, CORES, *T3), BF)
    D = jax.ShapeDtypeStruct((L, X, Y, Z, CORES, U, *T3), BF)
    og, ou, od = pl.pallas_call(
        place_kernel, out_shape=(G, G, D), in_specs=[VM], out_specs=(ANY,) * 3, scratch_shapes=[DMA((16,))],
        compiler_params=pltpu.CompilerParams(vmem_limit_bytes=2**20), name="place",
    )(pinned(VO, VMEM))
    return og, ou, od


def solution(mesh):
    def step(*arrays):
        terms, weights, m, v = (arrays[i : i + 3] for i in range(0, 12, 3))
        moments = [f(a) for a, f in zip((*m, *v), (view_m, view_m, view_md) * 2)]
        *sums, _ = rs_call([t[0] for t in terms], weights, moments)
        Wgu, Wd, new = up_call(sums, weights, moments)
        whole = [untiled(a, *w.shape[1:]) for a, w in zip(ag_call(Wgu, Wd), weights)]
        return (*whole, *new)

    all_of, cut = P(None, None, None), P(None, "dp", None)
    return jax.shard_map(
        step,
        mesh=mesh,
        in_specs=(P(("rep", "dp"), None, None, None),) * 3 + (all_of,) * 3 + (cut,) * 6,
        out_specs=(P("rep", None, None),) * 3 + (P("rep", "dp", None),) * 6,
        check_vma=False,
    )
```

```python
import functools

import jax
import jax.numpy as jnp
from jax import lax
from jax.experimental import pallas as pl
from jax.experimental.pallas import tpu as pltpu
from jax.sharding import PartitionSpec as P

MESH = pl.DeviceIdType.MESH
BF, F32 = jnp.bfloat16, jnp.float32
DMA = pltpu.SemaphoreType.DMA
VMEM, HBM = pltpu.VMEM, pltpu.HBM
ALL = slice(None)
L, X, Y, Z, U, CORES = 2, 2, 2, 4, 9, 2
N = X * Y * Z * CORES
SUB, ROWS, LANES = 8, 16, 128
T3 = (U, ROWS, LANES)
NP = 3 * L
HALF = NP - L
OWN = 5
PART = {'A': pl.ds(0, OWN), 'B': pl.ds(OWN, 3), 'C': U - 1}
BLOCK, TILES = 36, 36
RUN = TILES * L
MOMENTS = (2, 2, OWN * SUB, TILES, L, LANES)
VM, HB, ANY = (pl.BlockSpec(memory_space=s) for s in (VMEM, HBM, pl.ANY))


def tiled(a):
    l, r, c = a.shape
    return a.reshape(l, r // SUB, SUB, c // LANES, LANES).swapaxes(2, 3)


def untiled(a, r, c):
    return a.reshape(L, r // SUB, c // LANES, SUB, LANES).swapaxes(2, 3).reshape(L, r, c)


def view_gu(g): return tiled(g).reshape(L, X, Y, Z, U, CORES, *T3)
def view_d(g): return tiled(g).reshape(L, X, Y, Z, CORES, U, *T3)


def place():
    d = lax.axis_index("dp")
    d, c = d // CORES, d % CORES
    d, z = d // Z, d % Z
    return d // Y, d % Y, z, c


def dev(x, y, z, c): return 0, ((x * Y + y) * Z + z) * CORES + c


def line(z):
    h = z // 2
    return (z == 1) | (z == 2), [z, 1 - z + Z * h, 2 - h, 3 - 3 * h], z + 1 - 2 * h, 3 * h


def over(n, f): lax.fori_loop(0, n, lambda i, _: (f(i), 0)[1], 0)


def copy(src, dst, sem): return pltpu.make_async_copy(src, dst, sem)


def remote(src, dst, ss, rs, to): return pltpu.make_async_remote_copy(src, dst, ss, rs, device_id=to, device_id_type=MESH)


def got(ref, sem): copy(ref, ref, sem).wait()


def greet(to, mid, too):
    barrier = pltpu.get_barrier_semaphore()
    def signal(one): pl.semaphore_signal(barrier, 1, device_id=one, device_id_type=MESH)
    for one in to: signal(one)
    @pl.when(mid)
    def _(): signal(too)
    return lambda: pl.semaphore_wait(barrier, len(to) + mid.astype(jnp.int32))


def pinned(a, space): return pltpu.with_memory_space_constraint(a, space)


def split(name): return name[0], name[1], int(name[-1]) if name[-1].isdigit() else 0


def lagged(orders): return [[(n.rstrip('+'), n.count('+')) for n in names] for names in orders]


RS_ORDER = [
    ['Cz0', 'By0', 'Ax0', 'Cz2', 'Az0+', 'By1', 'Cz1', 'Ay1+', 'Ax4', 'Ax5', 'Ay3++', 'Az2++', 'By2', 'Bz0', 'Cy++', 'Ay2+', 'Az1+', 'Ax1', 'Ay0', 'Bx++', 'Ax2', 'By3+', 'Ax6+', 'Cx+', 'Ax7+', 'Af++', 'Bz1', 'Bz2+', 'Cf++', 'Ax3', 'Bf++'],
    ['Cz1+', 'Cz2+', 'By1', 'Ax0', 'Ax1', 'Ay2+', 'Ax7++', 'Az1++', 'By0', 'Ax2', 'Ay0', 'Bz1+', 'Az2++', 'Cz0', 'Cy++', 'Ax4', 'Ax3', 'Bx++', 'By3+', 'Ax6+', 'By2', 'Bz2+', 'Az0+', 'Ax5', 'Ay1', 'Ay3+', 'Cx+', 'Bz0', 'Af++', 'Cf++', 'Bf++'],
]
AHEAD = 5
CLASSES = {
    'A': ((OWN,), ['Ax0', 'Ax1', 'Ax2', 'Ax3', 'Ax4', 'Ax5', 'Ax6', 'Ax7', 'Ay0', 'Ay1', 'Ay2', 'Ay3', 'Az0', 'Az1', 'Az2', 'Af']),
    'By': ((X, 3), ['By0', 'By1', 'By2', 'By3', 'Bz0', 'Bz1', 'Bz2']),
    'Bx': ((3,), ['Bx', 'Bf']),
    'Cz': ((X, Y), ['Cz0', 'Cz1', 'Cz2']),
    'Cx': ((Y,), ['Cx']),
    'Cy': ((), ['Cy', 'Cf']),
}
CLASS_OF = {n: (k, i) for k, (_, names) in CLASSES.items() for i, n in enumerate(names)}
ARRIVE = {'Ax': (8, 'A'), 'Ay': (Z, 'A'), 'Az': (5, 'A'), 'By': (Z, 'By'), 'Bz': (5, 'By'), 'Bx': (1, 'Bx'), 'Cz': (5, 'Cz'), 'Cx': (1, 'Cx'), 'Cy': (1, 'Cy')}
LAST, CROSS = 2, 4


def rs_kernel(orders, gg, gu, gd, wg, wu, *refs):
    moments, (Ggu, Gd, TOT, MOM, DOWN, WGU, PARTNER), scr = refs[:6], refs[6:13], iter(refs[13:])
    take = lambda names: {n: next(scr) for n in names}
    own, par, snd, rcv = take(CLASSES), take(CLASSES), take(CLASSES), take(ARRIVE)
    fin, acc, sall = take(range(3)).values()
    own_s, par_s, snd_s, first_s, rcv_s = take(CLASSES), take(CLASSES), take(CLASSES), take(CLASSES), take(ARRIVE)
    d2d_ss, d2d_rs, gx_ss, gx_rs, sa_ss, sa_rs, mom_s = take(range(7)).values()
    x, y, z, c = place()
    ox, oy, oc = 1 - x, 1 - y, 1 - c
    me = lax.axis_index("dp")
    mid, near, inner, end = line(z)
    zo = near[::-1]
    side = z + 1 - 2 * (z % 2)
    NX, NY, NC = dev(ox, y, z, c), dev(x, oy, z, c), dev(x, y, z, oc)

    def block(name):
        n, axis, i = split(name)
        u = PART[n]
        if axis == 'f': return x, y, z, u
        if n == 'A':
            if axis == 'x': return ox, (oy if i < Z else y), zo[i % Z], u
            return x, (oy if axis == 'y' else y), zo[i], u
        if n == 'B':
            if axis == 'x': return ox, y, z, u
            return ALL, (oy if axis == 'y' else y), zo[i], u
        return {'z': (ALL, ALL, zo[i], u), 'x': (ox, ALL, z, u), 'y': (x, oy, z, u)}[axis]

    def cut(k, l, b, core):
        return gd.at[(l, *b[:3], core, b[3])] if k == 2 else (gg, gu)[k].at[(l, *b, core)]

    def reload(name, p):
        cl, i = CLASS_OF[name]
        b = block(name)
        @pl.when((p >= 0) & (p < NP))
        def _():
            for k in range(3):
                @pl.when(p // L == k)
                def _(): copy(cut(k, p % L, b, c), own[cl].at[i], own_s[cl].at[i]).start()
            @pl.when(p > 0)
            def _(): copy(PARTNER.at[(p, *b)], par[cl].at[i], par_s[cl].at[i]).start()

    def send(name, p, middle):
        cl, i = CLASS_OF[name]
        n, axis, j = split(name)
        if axis == 'x': to, slot = NX, j
        elif axis == 'y': to, slot = NY, j
        elif j < 2: to, slot = dev(x, y, inner, c), j + 3 * middle
        else: to, slot = dev(x, y, side, c), LAST
        kind = name[:2]
        return remote(snd[cl].at[i], rcv[kind].at[p, slot], snd_s[cl].at[i], rcv_s[kind].at[p, slot], to)

    def add(dst, refs, lead, last):
        def one(*idx):
            at = idx if idx else ...
            t = sum(r[at].astype(F32) for r in refs).astype(BF)
            dst[at] = t
            if last:
                t = t.astype(F32)
                acc[...] += jnp.sum(t * t, axis=0)
        if not lead: one()
        elif len(lead) == 1: over(lead[0], one)
        else: over(lead[0], lambda i: over(lead[1], lambda j: one(i, j)))

    def task(name, p, middle):
        cl, i = CLASS_OF[name]
        n, axis, j = split(name)
        lead = CLASSES[cl][0]
        R = lambda kind, s: rcv[kind].at[p, s]
        def arrive(*which):
            for kind, s in which: got(R(kind, s), rcv_s[kind].at[p, s])
        got(own[cl].at[i], own_s[cl].at[i])
        got(par[cl].at[i], par_s[cl].at[i])
        zk, refs, far, wait, farwait = n + 'z', [], [], [], []
        if axis == 'z':
            s = (0, 1, 3)[j]
            far, farwait = [R(zk, s)], [(zk, s)]
            wait = {'A': [('Ax', Z + j), ('Ay', j)], 'B': [('By', j)], 'C': []}[n]
            refs = [R(*w) for w in wait]
        elif name[:2] == 'Ay':
            wait = [('Ax', j)]
            refs = [R(*w) for w in wait]
        elif name == 'Af':
            wait, farwait = [('Ax', Z + 3), ('Ay', 3), (zk, LAST)], [(zk, CROSS)]
            refs, far = [R(*w) for w in wait], [R(zk, CROSS)]
        elif axis != 'y' or n == 'C':
            if n == 'B' and axis == 'x' or n == 'C' and axis == 'x': wait, farwait = [(zk, LAST)], [(zk, CROSS)]
            if name == 'Bx': wait += [('By', 3)]
            if name in ('Bf', 'Cy'): wait = [(n + 'x', 0)]
            if name == 'Cf': wait = [('Cy', 0)]
            here = {'Bx': (ox,), 'Bf': (x,), 'Cx': (ox,), 'Cy': (x, oy), 'Cf': (x, y)}.get(name)
            if here:
                refs, far = [R(zk, LAST).at[here]], [R(zk, CROSS).at[here]]
                if n == 'B': refs += [R('By', 3).at[here]]
                if name == 'Bf': refs += [R('Bx', 0)]
                if name == 'Cy': refs += [R('Cx', 0).at[oy]]
                if name == 'Cf': refs += [R('Cx', 0).at[y], R('Cy', 0)]
        arrive(*wait, *(farwait if middle else []))
        last = axis == 'f'
        if last: dst = fin.at[p, PART[n]]
        else:
            @pl.when(p > 0)
            def _(): send(name, p, middle).wait_send()
            dst = snd[cl].at[i]
        add(dst, [own[cl].at[i], par[cl].at[i]] + refs + (far if middle else []), lead, last)
        if not last: send(name, p, middle).start()

    def swap0(name):
        cl, i = CLASS_OF[name]
        return remote(cut(0, 0, block(name), oc), par[cl].at[i], first_s[cl].at[i], par_s[cl].at[i], NC)

    def swap(p):
        parts = [(ox, ALL, ALL, PART['A']), (ALL, ALL, ALL, PART['B']), (ALL, ALL, ALL, PART['C']), (x, ALL, ALL, PART['A'])]
        return [remote(cut(p // L, p % L, q, oc), PARTNER.at[(p, *q)], d2d_ss.at[p, i], d2d_rs.at[p, i], NC) for i, q in enumerate(parts)]

    met = greet((NX, NY, NC, dev(x, y, inner, c)), mid, dev(x, y, end, c))
    acc[...] = jnp.zeros_like(acc)
    for n in CLASS_OF: reload(n, jnp.int32(0))
    def others(f):
        def one(i):
            @pl.when(i != me)
            def _(): f((0, i))
        over(N, one)
    met()
    def both(f):
        for middle, order in enumerate(orders):
            @pl.when(mid if middle else jnp.logical_not(mid))
            def _(): f(order, middle)
    def swaps0(order, middle):
        for n, _ in sorted(order, key=lambda t: t[1]): swap0(n).start()
    both(swaps0)
    for p in range(1, NP):
        for cp in swap(p): cp.start()

    def rows(p): return remote(fin.at[p, pl.ds(Z * oc, OWN)], Ggu.at[p // L, p % L, :, c], gx_ss.at[p], gx_rs.at[p], NC)
    early = [copy(moments[k + 3 * i], MOM.at[k, i, pl.ds(Z * c, BLOCK)], mom_s.at[k, i]) for k in range(2) for i in range(2)]
    early += [copy(moments[2 + 3 * i], DOWN.at[i], mom_s.at[2, i]) for i in range(2)]
    early += [copy((wg, wu)[k].at[:, x, y, z, pl.ds(Z * c, OWN)], WGU.at[k], mom_s.at[3, k]) for k in range(2)]
    def part_of(name): return {'B': 1, 'C': 2}.get(name[0], 0 if name[1] == 'x' else 3)
    def round_(r, order, middle):
        heads = {}
        for lag in range(3):
            for n, own_lag in order:
                if own_lag == lag: heads.setdefault(part_of(n), n)
        for i, (n, lag) in enumerate(order):
            m, ml = order[(i + AHEAD) % len(order)]
            q = r + (i + AHEAD) // len(order) - ml
            @pl.when((q > 0) & (q < NP))
            def _():
                if heads[part_of(m)] == m:
                    for k in range(1, NP):
                        @pl.when(q == k)
                        def _(): swap(k)[part_of(m)].wait_recv()
                reload(m, q)
            p = r - lag
            @pl.when((p >= 0) & (p < NP))
            def _(): task(n, p, middle)
        q = r - max(lag for n, lag in order if n[1] == 'f')
        @pl.when((q >= 0) & (q < HALF))
        def _(): rows(q).start()
    def rounds(r):
        @pl.when(r == 1)
        def _():
            for cp in early: cp.start()
        both(functools.partial(round_, r))
    over(NP + max(lag for order in orders for _, lag in order), rounds)

    sall[me] = acc[0:SUB] + acc[SUB:ROWS]
    others(lambda to: remote(sall.at[me], sall.at[me], sa_ss, sa_rs, to).start())
    for l in range(L): Gd[l] = fin[HALF + l]
    for k in range(2):
        for i in range(2):
            MOM[k, i, pl.ds(BLOCK * oc, Z)] = jnp.zeros((Z, TILES, L, LANES), F32)
    for cp in early: cp.wait()
    for p in range(HALF):
        k, l = p // L, p % L
        Ggu[k, l, :, c] = fin[p, pl.ds(Z * c, OWN)]
        rows(p).wait()
    for n in CLASS_OF:
        swap0(n).wait_send()
        if n[1] != 'f': send(n, NP - 1, 0).wait_send()
    for p in range(1, NP):
        for cp in swap(p): cp.wait_send()
    rest = sall.at[pl.ds(0, N - 1)]
    got(rest, sa_rs)
    got(rest, sa_ss)
    TOT[...] = jnp.sum(sall[...], axis=0)


def rs_call(terms, weights, moments):
    bufs = [VMEM((len(names), *shape, *T3), BF) for shape, names in CLASSES.values()]
    sems = [DMA((len(names),)) for _, names in CLASSES.values()]
    scratch = bufs * 3 + [VMEM((NP, n, *CLASSES[cl][0], *T3), BF) for n, cl in ARRIVE.values()]
    scratch += [VMEM((NP, U, *T3), BF), VMEM((ROWS, LANES), F32), VMEM((N, SUB, LANES), F32)]
    scratch += sems * 4 + [DMA((NP, n)) for n, _ in ARRIVE.values()]
    scratch += [DMA((NP, 4)), DMA((NP, 4)), DMA((HALF,)), DMA((HALF,)), DMA(()), DMA(()), DMA((4, 2))]
    views = view_gu, view_gu, view_d
    return pl.pallas_call(
        functools.partial(rs_kernel, lagged(RS_ORDER)),
        out_shape=(VMEM((2, L, OWN, CORES, *T3), BF), VMEM((L, U, *T3), BF), VMEM((SUB, LANES), F32), VMEM(MOMENTS, F32), VMEM((2, L, U, *T3), F32), VMEM((2, L, OWN, CORES, *T3), BF), HBM((NP, X, Y, Z, U, *T3), BF)),
        in_specs=[HB] * 11,
        out_specs=(VM,) * 6 + (HB,),
        scratch_shapes=scratch,
        compiler_params=pltpu.CompilerParams(collective_id=0, has_side_effects=True, vmem_limit_bytes=54_800_000),
        name="reduce_scatter",
    )(*(pinned(a, HBM) for a in (*(f(a) for f, a in zip(views * 2, (*terms, *weights[:2]))), *moments)))


def up_kernel(count, Ggu, Gd, TOT, MOM, DOWN, WGU, wd, Wgu, Wd, *refs):
    new, (mom, down, wb, wdb, ld, st, ds) = refs[:6], refs[6:]
    x, y, z, c = place()
    load = copy(wd.at[:, x, y, z, c], wdb, ld)
    load.start()
    stores = []
    def store(src, dst):
        stores.append(copy(src, dst, st.at[len(stores)]))
        stores[-1].start()
    s = jnp.sum(jnp.sum(TOT[...], axis=0, keepdims=True), axis=1, keepdims=True)
    factor = jnp.minimum(1.0, 0.5 * lax.rsqrt(s * (1.0 / count) + 1e-30))
    def adamw(w, m, v, g):
        g = g * factor
        m = 0.9 * m + 0.1 * g
        v = 0.95 * v + 0.05 * g * g
        return w - 0.02 * (m * lax.rsqrt(v + 1e-8) + 0.1 * w), m, v
    def do_down():
        load.wait()
        def layer(l):
            def unit(u):
                for j in range(U):
                    at = (l, u, j)
                    w, m, v = adamw(wdb[at].astype(F32), DOWN[(0, *at)], DOWN[(1, *at)], Gd[at].astype(F32))
                    wdb[at] = w.astype(BF)
                    down[(0, *at)], down[(1, *at)] = m, v
            over(U, unit)
            for i in range(2): copy(down.at[i, l], new[2 + 3 * i].at[l], ds.at[i, l]).start()
        over(L, layer)
        store(wdb, Wd)
    for k in range(2):
        flat = lambda ref, i: ref.at[k, i].reshape(OWN * SUB * RUN, LANES)
        M, V, newM, newV = flat(MOM, 0), flat(MOM, 1), flat(mom, 0), flat(mom, 1)
        def tile(l, u, ch):
            base = SUB * u * RUN + TILES * ch + l
            for j in range(U):
                g, w = Ggu[k, l, u, ch, j].astype(F32), WGU[k, l, u, ch, j].astype(F32)
                half = []
                for e in range(2):
                    at = pl.ds(base + (2 * j + e) * L, SUB, stride=RUN)
                    h = slice(SUB * e, SUB * e + SUB)
                    wn, newM[at, :], newV[at, :] = adamw(w[h], M[at, :], V[at, :], g[h])
                    half.append(wn)
                wb[k, l, u, ch, j] = jnp.concatenate(half).astype(BF)
        for u in range(OWN):
            over(L, lambda l: [tile(l, u, ch) for ch in range(CORES)])
            row = max(SUB * u - Z, 0)
            n = Z if u == 0 else SUB
            for i in range(2): store(mom.at[k, i, pl.ds(Z * c + row, n)], new[k + 3 * i].at[pl.ds(row, n)])
            store(wb.at[k, :, u], Wgu.at[pl.ds(L * k, L), u])
        if k == 0: do_down()
    for cp in stores: cp.wait()
    for l in range(L):
        for i in range(2): copy(down.at[i, l], new[2 + 3 * i].at[l], ds.at[i, l]).wait()


def view_m(m): return m.reshape(L, BLOCK, TILES, LANES).transpose(1, 2, 0, 3)
def unview_m(m): return m.transpose(2, 0, 1, 3).reshape(L, BLOCK, TILES * LANES)
def view_md(m): return tiled(m).reshape(L, U, *T3)


def up_call(sums, weights, moments):
    count = sum(w.size for w in weights)
    W, Wd = (HALF, OWN, CORES, *T3), (L, U, *T3)
    res = pl.pallas_call(
        functools.partial(up_kernel, count),
        out_shape=(HBM(W, BF), HBM(Wd, BF), *(HBM(a.shape, F32) for a in moments)),
        in_specs=[VM] * 6 + [HB],
        out_specs=[HB] * 8,
        scratch_shapes=[VMEM(MOMENTS, F32), VMEM((2, *Wd), F32), VMEM((2, L, *W[1:]), BF), VMEM(Wd, BF), DMA(()), DMA((6 * OWN + 1,)), DMA((2, L))],
        compiler_params=pltpu.CompilerParams(vmem_limit_bytes=20 * 2**20),
        name="update",
    )(*(pinned(a, VMEM) for a in sums), pinned(view_d(weights[2]), HBM))
    rows, columns = weights[2].shape[1:]
    unview = (unview_m, unview_m, lambda a: untiled(a, rows // N, columns))
    new = [f(a) for a, f in zip(res[2:], unview * 2)]
    return res[0], res[1], new


AG_ORDER = [
    ['Bo', 'Co', 'Ax0_0++', 'Ao', 'Cx+', 'By_0++', 'Az_2+', 'Ay_1+', 'Ax0_3++', 'Bz_3++', 'By_1++', 'Bz_1+', 'Cy', 'Ax1_1++', 'Ay_3++', 'Cz_2++', 'Ax0_2++', 'Cz_1++', 'Az_3+', 'Bx', 'By_2++', 'Bz_2+', 'Ay_2+', 'Ax1_2++', 'Ax1_0+', 'Ax0_1+', 'Ay_0', 'Ax1_3++', 'Az_1', 'Cz_3++', 'By_3++'],
    ['Co', 'Bo+', 'Bz_3++', 'Ao', 'Az_2+', 'Az_1+', 'Ay_2++', 'Cx++', 'Ax0_0+', 'Cz_2++', 'Bx+', 'Ay_3++', 'Ax0_3++', 'Az_3+', 'Cz_3++', 'By_2++', 'Cy+', 'Bz_1+', 'Ax1_1++', 'Ay_1+', 'By_0++', 'Bz_2+', 'Ay_0+', 'Ax0_2++', 'By_1++', 'Ax1_0++', 'Ax0_1++', 'Ax1_2++', 'Ax1_3++', 'Cz_1+', 'By_3++'],
]


def ag_kernel(orders, wgu, wd, VO, tmp, own_s, ex_ss, ex_rs, xs, ys, zis, zos, ds, dr, axr, ayr, azr, byr, bzr, bxr, czr, cxr, cyr):
    x, y, z, c = place()
    ox, oy, oc = 1 - x, 1 - y, 1 - c
    mid, sl, inner, end = line(z)
    NX, NY, NC, ZI, ZO = dev(ox, y, z, c), dev(x, oy, z, c), dev(x, y, z, oc), dev(x, y, inner, c), dev(x, y, end, c)
    zr = {'A': azr, 'B': bzr, 'C': czr}

    def task(name, p, middle):
        n, axis, i = split(name)
        zz = sl[i]
        def at(idx): return VO.at[(p, *idx, PART[n], c)]
        def push(idx, to, ss, rs): remote(at(idx), at(idx), ss.at[p], rs, to).start()
        def give(idx): push(idx, NC, ds, dr.at[p])
        def chain(idx):
            rs = zr[n].at[p, zz]
            if i == 0 or middle and i == 1: push(idx, ZI, zis, rs)
            if middle and i != 1: push(idx, ZO, zos, rs)
        if axis == 'o':
            here = x, y, z
            if n == 'A':
                chain(here)
                push(here, NY, ys, ayr.at[p, z])
                push(here, NX, xs, axr.at[p, z, 0])
            elif n == 'B': push(here, NX, xs, bxr.at[p])
            else: push(here, NY, ys, cyr.at[p])
            give(here)
        elif n == 'A':
            if axis == 'z':
                here = x, y, zz
                got(at(here), azr.at[p, zz])
                chain(here)
                push(here, NY, ys, ayr.at[p, zz])
                push(here, NX, xs, axr.at[p, zz, 0])
            elif axis == 'y':
                here = x, oy, zz
                got(at(here), ayr.at[p, zz])
                push(here, NX, xs, axr.at[p, zz, 1])
            else:
                k = int(name[2])
                here = ox, (oy if k else y), zz
                got(at(here), axr.at[p, zz, k])
            give(here)
        elif n == 'B':
            here, wide = (ox, y, z), (ALL, y, zz)
            if axis == 'y':
                here = ALL, oy, zz
                got(at(here), byr.at[p, zz])
            else:
                if axis == 'x': got(at(here), bxr.at[p])
                else:
                    here = wide
                    got(at(here), bzr.at[p, zz])
                chain(wide)
                push(wide, NY, ys, byr.at[p, zz])
            give(here)
        elif axis == 'y':
            here = x, oy, z
            got(at(here), cyr.at[p])
            push((x, ALL, z), NX, xs, cxr.at[p])
            give(here)
        else:
            here, wide = (ox, ALL, z), (ALL, ALL, zz)
            if axis == 'x': got(at(here), cxr.at[p])
            else:
                here = wide
                got(at(here), czr.at[p, zz])
            chain(wide)
            give(here)

    met = greet((NX, NY, NC, ZI), mid, ZO)
    mine = VO.at[:, x, y, z]
    own = [copy(wd.at[l], mine.at[l, :, c], own_s.at[l]) for l in range(L)]
    own += [copy(wgu.at[q, pl.ds(c, Z), c], mine.at[L + q, pl.ds(OWN * c, Z), c], own_s.at[L + q]) for q in range(HALF)]
    own += [copy(wgu.at[:, Z * oc, c], tmp.at[0], own_s.at[NP])]
    for cp in own: cp.start()
    met()
    swap = [remote(wgu.at[q, pl.ds(c, Z), oc], mine.at[L + q, pl.ds(OWN * c, Z), oc], ex_ss.at[q], ex_rs.at[q], NC) for q in range(HALF)]
    swap += [remote(wgu.at[:, Z * oc, oc], tmp.at[1], ex_ss.at[HALF], ex_rs.at[HALF], NC)]
    for cp in swap: cp.start()
    for cp in own[:L]: cp.wait()

    def round_(r):
        @pl.when(r == 1)
        def _():
            for cp in own[L:] + swap: cp.wait()
            upper = lax.broadcasted_iota(jnp.int32, T3, 1) % SUB < Z
            first = upper.astype(jnp.int32) == oc
            for q in range(HALF):
                VO[L + q, x, y, z, Z, c] = jnp.where(first, tmp[0, q].astype(F32), tmp[1, q].astype(F32)).astype(BF)
        for middle, order in enumerate(orders):
            @pl.when(mid if middle else jnp.logical_not(mid))
            def _():
                for n, lag in order:
                    p = r - lag
                    @pl.when((p >= 0) & (p < NP))
                    def _(): task(n, p, middle)
    over(NP + max(lag for order in orders for _, lag in order), round_)

    def finish(p):
        q = VO.at[pl.ds(0, 5), 0, 0, 0, :, 0]
        got(q, xs.at[p])
        got(q, ys.at[p])
        @pl.when(mid)
        def _():
            got(q.at[:, pl.ds(0, 6)], zis.at[p])
            got(q, zos.at[p])
        @pl.when(jnp.logical_not(mid))
        def _(): got(q.at[:, pl.ds(0, 3)], zis.at[p])
        whole = VO.at[0, :, :, :, :, 0]
        got(whole, ds.at[p])
        got(whole, dr.at[p])
    over(NP, finish)


def place_kernel(VO, og, ou, od, sems):
    out = []
    def put(src, dst):
        out.append(copy(src, dst, sems.at[len(out)]))
        out[-1].start()
    for l in range(L):
        for i in range(X):
            for k in range(CORES): put(VO.at[l, i, :, :, :, k], od.at[l, i, :, :, k])
            put(VO.at[L + l, i], og.at[l, i])
            put(VO.at[2 * L + l, i], ou.at[l, i])
    for cp in out: cp.wait()


def ag_call(wgu, wd):
    four = DMA((NP, Z))
    one = DMA((NP,))
    VO = pl.pallas_call(
        functools.partial(ag_kernel, lagged(AG_ORDER)),
        out_shape=VMEM((NP, X, Y, Z, U, CORES, *T3), BF),
        in_specs=[HB] * 2,
        out_specs=VM,
        scratch_shapes=[VMEM((2, HALF, *T3), BF), DMA((NP + 1,)), DMA((HALF + 1,)), DMA((HALF + 1,))] + [one] * 6 + [DMA((NP, Z, 2)), four, four, four, four, one, four, one, one],
        compiler_params=pltpu.CompilerParams(collective_id=1, has_side_effects=True, vmem_limit_bytes=2**20),
        name="all_gather",
    )(pinned(wgu, HBM), pinned(wd, HBM))
    G = jax.ShapeDtypeStruct((L, X, Y, Z, U, CORES, *T3), BF)
    D = jax.ShapeDtypeStruct((L, X, Y, Z, CORES, U, *T3), BF)
    og, ou, od = pl.pallas_call(
        place_kernel, out_shape=(G, G, D), in_specs=[VM], out_specs=(ANY,) * 3, scratch_shapes=[DMA((16,))],
        compiler_params=pltpu.CompilerParams(vmem_limit_bytes=2**20), name="place",
    )(pinned(VO, VMEM))
    return og, ou, od


def solution(mesh):
    def step(*arrays):
        terms, weights, m, v = (arrays[i : i + 3] for i in range(0, 12, 3))
        moments = [f(a) for a, f in zip((*m, *v), (view_m, view_m, view_md) * 2)]
        *sums, _ = rs_call([t[0] for t in terms], weights, moments)
        Wgu, Wd, new = up_call(sums, weights, moments)
        whole = [untiled(a, *w.shape[1:]) for a, w in zip(ag_call(Wgu, Wd), weights)]
        return (*whole, *new)

    all_of, cut = P(None, None, None), P(None, "dp", None)
    return jax.shard_map(
        step,
        mesh=mesh,
        in_specs=(P(("rep", "dp"), None, None, None),) * 3 + (all_of,) * 3 + (cut,) * 6,
        out_specs=(P("rep", None, None),) * 3 + (P("rep", "dp", None),) * 6,
        check_vma=False,
    )
```

```python
import functools

import jax
import jax.numpy as jnp
from jax import lax
from jax.experimental import pallas as pl
from jax.experimental.pallas import tpu as pltpu
from jax.sharding import PartitionSpec as P

MESH = pl.DeviceIdType.MESH
BF, F32 = jnp.bfloat16, jnp.float32
DMA = pltpu.SemaphoreType.DMA
VMEM, HBM = pltpu.VMEM, pltpu.HBM
ALL = slice(None)
L, X, Y, Z, U, CORES = 2, 2, 2, 4, 9, 2
N = X * Y * Z * CORES
SUB, ROWS, LANES = 8, 16, 128
T3 = (U, ROWS, LANES)
NP = 3 * L
HALF = NP - L
OWN = 5
PART = {'A': pl.ds(0, OWN), 'B': pl.ds(OWN, 3), 'C': U - 1}
BLOCK, TILES = 36, 36
RUN = TILES * L
MOMENTS = (2, 2, OWN * SUB, TILES, L, LANES)
VM, HB, ANY = (pl.BlockSpec(memory_space=s) for s in (VMEM, HBM, pl.ANY))


def tiled(a):
    l, r, c = a.shape
    return a.reshape(l, r // SUB, SUB, c // LANES, LANES).swapaxes(2, 3)


def untiled(a, r, c):
    return a.reshape(L, r // SUB, c // LANES, SUB, LANES).swapaxes(2, 3).reshape(L, r, c)


def view_gu(g): return tiled(g).reshape(L, X, Y, Z, U, CORES, *T3)
def view_d(g): return tiled(g).reshape(L, X, Y, Z, CORES, U, *T3)


def place():
    d = lax.axis_index("dp")
    d, c = d // CORES, d % CORES
    d, z = d // Z, d % Z
    return d // Y, d % Y, z, c


def dev(x, y, z, c): return 0, ((x * Y + y) * Z + z) * CORES + c


def line(z):
    h = z // 2
    return (z == 1) | (z == 2), [z, 1 - z + Z * h, 2 - h, 3 - 3 * h], z + 1 - 2 * h, 3 * h


def over(n, f): lax.fori_loop(0, n, lambda i, _: (f(i), 0)[1], 0)


def copy(src, dst, sem): return pltpu.make_async_copy(src, dst, sem)


def remote(src, dst, ss, rs, to): return pltpu.make_async_remote_copy(src, dst, ss, rs, device_id=to, device_id_type=MESH)


def got(ref, sem): copy(ref, ref, sem).wait()


def greet(to, mid, too):
    barrier = pltpu.get_barrier_semaphore()
    def signal(one): pl.semaphore_signal(barrier, 1, device_id=one, device_id_type=MESH)
    for one in to: signal(one)
    @pl.when(mid)
    def _(): signal(too)
    return lambda: pl.semaphore_wait(barrier, len(to) + mid.astype(jnp.int32))


def pinned(a, space): return pltpu.with_memory_space_constraint(a, space)


def split(name): return name[0], name[1], int(name[-1]) if name[-1].isdigit() else 0


def lagged(orders): return [[(n.rstrip('+'), n.count('+')) for n in names] for names in orders]


RS_ORDER = [
    ['Cz0', 'By0', 'Ax0', 'Cz2', 'Az0+', 'By1', 'Cz1', 'Ay1+', 'Ax4', 'Ax5', 'Ay3++', 'Az2++', 'By2', 'Bz0', 'Cy++', 'Ay2+', 'Az1+', 'Ax1', 'Ay0', 'Bx++', 'Ax2', 'By3+', 'Ax6+', 'Cx+', 'Ax7+', 'Af++', 'Bz1', 'Bz2+', 'Cf++', 'Ax3', 'Bf++'],
    ['Cz1+', 'Cz2+', 'By1', 'Ax0', 'Ax1', 'Ay2+', 'Ax7++', 'Az1++', 'By0', 'Ax2', 'Ay0', 'Bz1+', 'Az2++', 'Cz0', 'Cy++', 'Ax4', 'Ax3', 'Bx++', 'By3+', 'Ax6+', 'By2', 'Bz2+', 'Az0+', 'Ax5', 'Ay1', 'Ay3+', 'Cx+', 'Bz0', 'Af++', 'Cf++', 'Bf++'],
]
AHEAD = 5
CLASSES = {
    'A': ((OWN,), ['Ax0', 'Ax1', 'Ax2', 'Ax3', 'Ax4', 'Ax5', 'Ax6', 'Ax7', 'Ay0', 'Ay1', 'Ay2', 'Ay3', 'Az0', 'Az1', 'Az2', 'Af']),
    'By': ((X, 3), ['By0', 'By1', 'By2', 'By3', 'Bz0', 'Bz1', 'Bz2']),
    'Bx': ((3,), ['Bx', 'Bf']),
    'Cz': ((X, Y), ['Cz0', 'Cz1', 'Cz2']),
    'Cx': ((Y,), ['Cx']),
    'Cy': ((), ['Cy', 'Cf']),
}
CLASS_OF = {n: (k, i) for k, (_, names) in CLASSES.items() for i, n in enumerate(names)}
ARRIVE = {'Ax': (8, 'A'), 'Ay': (Z, 'A'), 'Az': (5, 'A'), 'By': (Z, 'By'), 'Bz': (5, 'By'), 'Bx': (1, 'Bx'), 'Cz': (5, 'Cz'), 'Cx': (1, 'Cx'), 'Cy': (1, 'Cy')}
LAST, CROSS = 2, 4


def rs_kernel(orders, gg, gu, gd, wg, wu, *refs):
    moments, (Ggu, Gd, TOT, MOM, DOWN, WGU, PARTNER), scr = refs[:6], refs[6:13], iter(refs[13:])
    take = lambda names: {n: next(scr) for n in names}
    own, par, snd, rcv = take(CLASSES), take(CLASSES), take(CLASSES), take(ARRIVE)
    fin, acc, sall = take(range(3)).values()
    own_s, par_s, snd_s, first_s, rcv_s = take(CLASSES), take(CLASSES), take(CLASSES), take(CLASSES), take(ARRIVE)
    d2d_ss, d2d_rs, gx_ss, gx_rs, sa_ss, sa_rs, mom_s = take(range(7)).values()
    x, y, z, c = place()
    ox, oy, oc = 1 - x, 1 - y, 1 - c
    me = lax.axis_index("dp")
    mid, near, inner, end = line(z)
    zo = near[::-1]
    side = z + 1 - 2 * (z % 2)
    NX, NY, NC = dev(ox, y, z, c), dev(x, oy, z, c), dev(x, y, z, oc)

    def block(name):
        n, axis, i = split(name)
        u = PART[n]
        if axis == 'f': return x, y, z, u
        if n == 'A':
            if axis == 'x': return ox, (oy if i < Z else y), zo[i % Z], u
            return x, (oy if axis == 'y' else y), zo[i], u
        if n == 'B':
            if axis == 'x': return ox, y, z, u
            return ALL, (oy if axis == 'y' else y), zo[i], u
        return {'z': (ALL, ALL, zo[i], u), 'x': (ox, ALL, z, u), 'y': (x, oy, z, u)}[axis]

    def cut(k, l, b, core):
        return gd.at[(l, *b[:3], core, b[3])] if k == 2 else (gg, gu)[k].at[(l, *b, core)]

    def reload(name, p):
        cl, i = CLASS_OF[name]
        b = block(name)
        @pl.when((p >= 0) & (p < NP))
        def _():
            for k in range(3):
                @pl.when(p // L == k)
                def _(): copy(cut(k, p % L, b, c), own[cl].at[i], own_s[cl].at[i]).start()
            @pl.when(p > 0)
            def _(): copy(PARTNER.at[(p, *b)], par[cl].at[i], par_s[cl].at[i]).start()

    def send(name, p, middle):
        cl, i = CLASS_OF[name]
        n, axis, j = split(name)
        if axis == 'x': to, slot = NX, j
        elif axis == 'y': to, slot = NY, j
        elif j < 2: to, slot = dev(x, y, inner, c), j + 3 * middle
        else: to, slot = dev(x, y, side, c), LAST
        kind = name[:2]
        return remote(snd[cl].at[i], rcv[kind].at[p, slot], snd_s[cl].at[i], rcv_s[kind].at[p, slot], to)

    def add(dst, refs, lead, last):
        def one(*idx):
            at = idx if idx else ...
            t = sum(r[at].astype(F32) for r in refs).astype(BF)
            dst[at] = t
            if last:
                t = t.astype(F32)
                acc[...] += jnp.sum(t * t, axis=0)
        if not lead: one()
        elif len(lead) == 1: over(lead[0], one)
        else: over(lead[0], lambda i: over(lead[1], lambda j: one(i, j)))

    def task(name, p, middle):
        cl, i = CLASS_OF[name]
        n, axis, j = split(name)
        lead = CLASSES[cl][0]
        R = lambda kind, s: rcv[kind].at[p, s]
        def arrive(*which):
            for kind, s in which: got(R(kind, s), rcv_s[kind].at[p, s])
        got(own[cl].at[i], own_s[cl].at[i])
        got(par[cl].at[i], par_s[cl].at[i])
        zk, refs, far, wait, farwait = n + 'z', [], [], [], []
        if axis == 'z':
            s = (0, 1, 3)[j]
            far, farwait = [R(zk, s)], [(zk, s)]
            wait = {'A': [('Ax', Z + j), ('Ay', j)], 'B': [('By', j)], 'C': []}[n]
            refs = [R(*w) for w in wait]
        elif name[:2] == 'Ay':
            wait = [('Ax', j)]
            refs = [R(*w) for w in wait]
        elif name == 'Af':
            wait, farwait = [('Ax', Z + 3), ('Ay', 3), (zk, LAST)], [(zk, CROSS)]
            refs, far = [R(*w) for w in wait], [R(zk, CROSS)]
        elif axis != 'y' or n == 'C':
            if n == 'B' and axis == 'x' or n == 'C' and axis == 'x': wait, farwait = [(zk, LAST)], [(zk, CROSS)]
            if name == 'Bx': wait += [('By', 3)]
            if name in ('Bf', 'Cy'): wait = [(n + 'x', 0)]
            if name == 'Cf': wait = [('Cy', 0)]
            here = {'Bx': (ox,), 'Bf': (x,), 'Cx': (ox,), 'Cy': (x, oy), 'Cf': (x, y)}.get(name)
            if here:
                refs, far = [R(zk, LAST).at[here]], [R(zk, CROSS).at[here]]
                if n == 'B': refs += [R('By', 3).at[here]]
                if name == 'Bf': refs += [R('Bx', 0)]
                if name == 'Cy': refs += [R('Cx', 0).at[oy]]
                if name == 'Cf': refs += [R('Cx', 0).at[y], R('Cy', 0)]
        arrive(*wait, *(farwait if middle else []))
        last = axis == 'f'
        if last: dst = fin.at[p, PART[n]]
        else:
            @pl.when(p > 0)
            def _(): send(name, p, middle).wait_send()
            dst = snd[cl].at[i]
        add(dst, [own[cl].at[i], par[cl].at[i]] + refs + (far if middle else []), lead, last)
        if not last: send(name, p, middle).start()

    def swap0(name):
        cl, i = CLASS_OF[name]
        return remote(cut(0, 0, block(name), oc), par[cl].at[i], first_s[cl].at[i], par_s[cl].at[i], NC)

    def swap(p):
        parts = [(ox, ALL, ALL, PART['A']), (ALL, ALL, ALL, PART['B']), (ALL, ALL, ALL, PART['C']), (x, ALL, ALL, PART['A'])]
        return [remote(cut(p // L, p % L, q, oc), PARTNER.at[(p, *q)], d2d_ss.at[p, i], d2d_rs.at[p, i], NC) for i, q in enumerate(parts)]

    met = greet((NX, NY, NC, dev(x, y, inner, c)), mid, dev(x, y, end, c))
    acc[...] = jnp.zeros_like(acc)
    for n in CLASS_OF: reload(n, jnp.int32(0))
    def others(f):
        def one(i):
            @pl.when(i != me)
            def _(): f((0, i))
        over(N, one)
    met()
    def both(f):
        for middle, order in enumerate(orders):
            @pl.when(mid if middle else jnp.logical_not(mid))
            def _(): f(order, middle)
    def swaps0(order, middle):
        for n, _ in sorted(order, key=lambda t: t[1]): swap0(n).start()
    both(swaps0)
    for p in range(1, NP):
        for cp in swap(p): cp.start()

    def rows(p): return remote(fin.at[p, pl.ds(Z * oc, OWN)], Ggu.at[p // L, p % L, :, c], gx_ss.at[p], gx_rs.at[p], NC)
    early = [copy(moments[k + 3 * i], MOM.at[k, i, pl.ds(Z * c, BLOCK)], mom_s.at[k, i]) for k in range(2) for i in range(2)]
    early += [copy(moments[2 + 3 * i], DOWN.at[i], mom_s.at[2, i]) for i in range(2)]
    early += [copy((wg, wu)[k].at[:, x, y, z, pl.ds(Z * c, OWN)], WGU.at[k], mom_s.at[3, k]) for k in range(2)]
    def part_of(name): return {'B': 1, 'C': 2}.get(name[0], 0 if name[1] == 'x' else 3)
    def round_(r, order, middle):
        heads = {}
        for lag in range(3):
            for n, own_lag in order:
                if own_lag == lag: heads.setdefault(part_of(n), n)
        for i, (n, lag) in enumerate(order):
            m, ml = order[(i + AHEAD) % len(order)]
            q = r + (i + AHEAD) // len(order) - ml
            @pl.when((q > 0) & (q < NP))
            def _():
                if heads[part_of(m)] == m:
                    for k in range(1, NP):
                        @pl.when(q == k)
                        def _(): swap(k)[part_of(m)].wait_recv()
                reload(m, q)
            p = r - lag
            @pl.when((p >= 0) & (p < NP))
            def _(): task(n, p, middle)
        q = r - max(lag for n, lag in order if n[1] == 'f')
        @pl.when((q >= 0) & (q < HALF))
        def _(): rows(q).start()
    def rounds(r):
        @pl.when(r == 1)
        def _():
            for cp in early: cp.start()
        both(functools.partial(round_, r))
    over(NP + max(lag for order in orders for _, lag in order), rounds)

    sall[me] = acc[0:SUB] + acc[SUB:ROWS]
    others(lambda to: remote(sall.at[me], sall.at[me], sa_ss, sa_rs, to).start())
    for l in range(L): Gd[l] = fin[HALF + l]
    for k in range(2):
        for i in range(2):
            MOM[k, i, pl.ds(BLOCK * oc, Z)] = jnp.zeros((Z, TILES, L, LANES), F32)
    for cp in early: cp.wait()
    for p in range(HALF):
        k, l = p // L, p % L
        Ggu[k, l, :, c] = fin[p, pl.ds(Z * c, OWN)]
        rows(p).wait()
    for n in CLASS_OF:
        swap0(n).wait_send()
        if n[1] != 'f': send(n, NP - 1, 0).wait_send()
    for p in range(1, NP):
        for cp in swap(p): cp.wait_send()
    rest = sall.at[pl.ds(0, N - 1)]
    got(rest, sa_rs)
    got(rest, sa_ss)
    TOT[...] = jnp.sum(sall[...], axis=0)


def rs_call(terms, weights, moments):
    bufs = [VMEM((len(names), *shape, *T3), BF) for shape, names in CLASSES.values()]
    sems = [DMA((len(names),)) for _, names in CLASSES.values()]
    scratch = bufs * 3 + [VMEM((NP, n, *CLASSES[cl][0], *T3), BF) for n, cl in ARRIVE.values()]
    scratch += [VMEM((NP, U, *T3), BF), VMEM((ROWS, LANES), F32), VMEM((N, SUB, LANES), F32)]
    scratch += sems * 4 + [DMA((NP, n)) for n, _ in ARRIVE.values()]
    scratch += [DMA((NP, 4)), DMA((NP, 4)), DMA((HALF,)), DMA((HALF,)), DMA(()), DMA(()), DMA((4, 2))]
    views = view_gu, view_gu, view_d
    return pl.pallas_call(
        functools.partial(rs_kernel, lagged(RS_ORDER)),
        out_shape=(VMEM((2, L, OWN, CORES, *T3), BF), VMEM((L, U, *T3), BF), VMEM((SUB, LANES), F32), VMEM(MOMENTS, F32), VMEM((2, L, U, *T3), F32), VMEM((2, L, OWN, CORES, *T3), BF), HBM((NP, X, Y, Z, U, *T3), BF)),
        in_specs=[HB] * 11,
        out_specs=(VM,) * 6 + (HB,),
        scratch_shapes=scratch,
        compiler_params=pltpu.CompilerParams(collective_id=0, has_side_effects=True, vmem_limit_bytes=54_800_000),
        name="reduce_scatter",
    )(*(pinned(a, HBM) for a in (*(f(a) for f, a in zip(views * 2, (*terms, *weights[:2]))), *moments)))


def up_kernel(count, Ggu, Gd, TOT, MOM, DOWN, WGU, wd, Wgu, Wd, *refs):
    new, (mom, down, wb, wdb, ld, st, ds) = refs[:6], refs[6:]
    x, y, z, c = place()
    load = copy(wd.at[:, x, y, z, c], wdb, ld)
    load.start()
    stores = []
    def store(src, dst):
        stores.append(copy(src, dst, st.at[len(stores)]))
        stores[-1].start()
    s = jnp.sum(jnp.sum(TOT[...], axis=0, keepdims=True), axis=1, keepdims=True)
    factor = jnp.minimum(1.0, 0.5 * lax.rsqrt(s * (1.0 / count) + 1e-30))
    def adamw(w, m, v, g):
        g = g * factor
        m = 0.9 * m + 0.1 * g
        v = 0.95 * v + 0.05 * g * g
        return w - 0.02 * (m * lax.rsqrt(v + 1e-8) + 0.1 * w), m, v
    def do_down():
        load.wait()
        def layer(l):
            def unit(u):
                for j in range(U):
                    at = (l, u, j)
                    w, m, v = adamw(wdb[at].astype(F32), DOWN[(0, *at)], DOWN[(1, *at)], Gd[at].astype(F32))
                    wdb[at] = w.astype(BF)
                    down[(0, *at)], down[(1, *at)] = m, v
            over(U, unit)
            for i in range(2): copy(down.at[i, l], new[2 + 3 * i].at[l], ds.at[i, l]).start()
        over(L, layer)
        store(wdb, Wd)
    for k in range(2):
        flat = lambda ref, i: ref.at[k, i].reshape(OWN * SUB * RUN, LANES)
        M, V, newM, newV = flat(MOM, 0), flat(MOM, 1), flat(mom, 0), flat(mom, 1)
        def tile(l, u, ch):
            base = SUB * u * RUN + TILES * ch + l
            for j in range(U):
                g, w = Ggu[k, l, u, ch, j].astype(F32), WGU[k, l, u, ch, j].astype(F32)
                half = []
                for e in range(2):
                    at = pl.ds(base + (2 * j + e) * L, SUB, stride=RUN)
                    h = slice(SUB * e, SUB * e + SUB)
                    wn, newM[at, :], newV[at, :] = adamw(w[h], M[at, :], V[at, :], g[h])
                    half.append(wn)
                wb[k, l, u, ch, j] = jnp.concatenate(half).astype(BF)
        for u in range(OWN):
            over(L, lambda l: [tile(l, u, ch) for ch in range(CORES)])
            row = max(SUB * u - Z, 0)
            n = Z if u == 0 else SUB
            for i in range(2): store(mom.at[k, i, pl.ds(Z * c + row, n)], new[k + 3 * i].at[pl.ds(row, n)])
            store(wb.at[k, :, u], Wgu.at[pl.ds(L * k, L), u])
        if k == 0: do_down()
    for cp in stores: cp.wait()
    for l in range(L):
        for i in range(2): copy(down.at[i, l], new[2 + 3 * i].at[l], ds.at[i, l]).wait()


def view_m(m): return m.reshape(L, BLOCK, TILES, LANES).transpose(1, 2, 0, 3)
def unview_m(m): return m.transpose(2, 0, 1, 3).reshape(L, BLOCK, TILES * LANES)
def view_md(m): return tiled(m).reshape(L, U, *T3)


def up_call(sums, weights, moments):
    count = sum(w.size for w in weights)
    W, Wd = (HALF, OWN, CORES, *T3), (L, U, *T3)
    res = pl.pallas_call(
        functools.partial(up_kernel, count),
        out_shape=(HBM(W, BF), HBM(Wd, BF), *(HBM(a.shape, F32) for a in moments)),
        in_specs=[VM] * 6 + [HB],
        out_specs=[HB] * 8,
        scratch_shapes=[VMEM(MOMENTS, F32), VMEM((2, *Wd), F32), VMEM((2, L, *W[1:]), BF), VMEM(Wd, BF), DMA(()), DMA((6 * OWN + 1,)), DMA((2, L))],
        compiler_params=pltpu.CompilerParams(vmem_limit_bytes=20 * 2**20),
        name="update",
    )(*(pinned(a, VMEM) for a in sums), pinned(view_d(weights[2]), HBM))
    rows, columns = weights[2].shape[1:]
    unview = (unview_m, unview_m, lambda a: untiled(a, rows // N, columns))
    new = [f(a) for a, f in zip(res[2:], unview * 2)]
    return res[0], res[1], new


AG_ORDER = [
    ['Bo', 'Co', 'Ax0_0++', 'Ao', 'Cx+', 'By_0++', 'Az_2+', 'Ay_1+', 'Ax0_3++', 'Bz_3++', 'By_1++', 'Bz_1+', 'Cy', 'Ax1_1++', 'Ay_3++', 'Cz_2++', 'Ax0_2++', 'Cz_1++', 'Az_3+', 'Bx', 'By_2++', 'Bz_2+', 'Ay_2+', 'Ax1_2++', 'Ax1_0+', 'Ax0_1+', 'Ay_0', 'Ax1_3++', 'Az_1', 'Cz_3++', 'By_3++'],
    ['Co', 'Bo+', 'Bz_3++', 'Ao', 'Az_2+', 'Az_1+', 'Ay_2++', 'Cx++', 'Ax0_0+', 'Cz_2++', 'Bx+', 'Ay_3++', 'Ax0_3++', 'Az_3+', 'Cz_3++', 'By_2++', 'Cy+', 'Bz_1+', 'Ax1_1++', 'Ay_1+', 'By_0++', 'Bz_2+', 'Ay_0+', 'Ax0_2++', 'By_1++', 'Ax1_0++', 'Ax0_1++', 'Ax1_2++', 'Ax1_3++', 'Cz_1+', 'By_3++'],
]


def ag_kernel(orders, wgu, wd, VO, tmp, own_s, ex_ss, ex_rs, xs, ys, zis, zos, ds, dr, axr, ayr, azr, byr, bzr, bxr, czr, cxr, cyr):
    x, y, z, c = place()
    ox, oy, oc = 1 - x, 1 - y, 1 - c
    mid, sl, inner, end = line(z)
    NX, NY, NC, ZI, ZO = dev(ox, y, z, c), dev(x, oy, z, c), dev(x, y, z, oc), dev(x, y, inner, c), dev(x, y, end, c)
    zr = {'A': azr, 'B': bzr, 'C': czr}

    def task(name, p, middle):
        n, axis, i = split(name)
        zz = sl[i]
        def at(idx): return VO.at[(p, *idx, PART[n], c)]
        def push(idx, to, ss, rs): remote(at(idx), at(idx), ss.at[p], rs, to).start()
        def give(idx): push(idx, NC, ds, dr.at[p])
        def chain(idx):
            rs = zr[n].at[p, zz]
            if i == 0 or middle and i == 1: push(idx, ZI, zis, rs)
            if middle and i != 1: push(idx, ZO, zos, rs)
        if axis == 'o':
            here = x, y, z
            if n == 'A':
                chain(here)
                push(here, NY, ys, ayr.at[p, z])
                push(here, NX, xs, axr.at[p, z, 0])
            elif n == 'B': push(here, NX, xs, bxr.at[p])
            else: push(here, NY, ys, cyr.at[p])
            give(here)
        elif n == 'A':
            if axis == 'z':
                here = x, y, zz
                got(at(here), azr.at[p, zz])
                chain(here)
                push(here, NY, ys, ayr.at[p, zz])
                push(here, NX, xs, axr.at[p, zz, 0])
            elif axis == 'y':
                here = x, oy, zz
                got(at(here), ayr.at[p, zz])
                push(here, NX, xs, axr.at[p, zz, 1])
            else:
                k = int(name[2])
                here = ox, (oy if k else y), zz
                got(at(here), axr.at[p, zz, k])
            give(here)
        elif n == 'B':
            here, wide = (ox, y, z), (ALL, y, zz)
            if axis == 'y':
                here = ALL, oy, zz
                got(at(here), byr.at[p, zz])
            else:
                if axis == 'x': got(at(here), bxr.at[p])
                else:
                    here = wide
                    got(at(here), bzr.at[p, zz])
                chain(wide)
                push(wide, NY, ys, byr.at[p, zz])
            give(here)
        elif axis == 'y':
            here = x, oy, z
            got(at(here), cyr.at[p])
            push((x, ALL, z), NX, xs, cxr.at[p])
            give(here)
        else:
            here, wide = (ox, ALL, z), (ALL, ALL, zz)
            if axis == 'x': got(at(here), cxr.at[p])
            else:
                here = wide
                got(at(here), czr.at[p, zz])
            chain(wide)
            give(here)

    met = greet((NX, NY, NC, ZI), mid, ZO)
    mine = VO.at[:, x, y, z]
    own = [copy(wd.at[l], mine.at[l, :, c], own_s.at[l]) for l in range(L)]
    own += [copy(wgu.at[q, pl.ds(c, Z), c], mine.at[L + q, pl.ds(OWN * c, Z), c], own_s.at[L + q]) for q in range(HALF)]
    own += [copy(wgu.at[:, Z * oc, c], tmp.at[0], own_s.at[NP])]
    for cp in own: cp.start()
    met()
    swap = [remote(wgu.at[q, pl.ds(c, Z), oc], mine.at[L + q, pl.ds(OWN * c, Z), oc], ex_ss.at[q], ex_rs.at[q], NC) for q in range(HALF)]
    swap += [remote(wgu.at[:, Z * oc, oc], tmp.at[1], ex_ss.at[HALF], ex_rs.at[HALF], NC)]
    for cp in swap: cp.start()
    for cp in own[:L]: cp.wait()

    def round_(r):
        @pl.when(r == 1)
        def _():
            for cp in own[L:] + swap: cp.wait()
            upper = lax.broadcasted_iota(jnp.int32, T3, 1) % SUB < Z
            first = upper.astype(jnp.int32) == oc
            for q in range(HALF):
                VO[L + q, x, y, z, Z, c] = jnp.where(first, tmp[0, q].astype(F32), tmp[1, q].astype(F32)).astype(BF)
        for middle, order in enumerate(orders):
            @pl.when(mid if middle else jnp.logical_not(mid))
            def _():
                for n, lag in order:
                    p = r - lag
                    @pl.when((p >= 0) & (p < NP))
                    def _(): task(n, p, middle)
    over(NP + max(lag for order in orders for _, lag in order), round_)

    def finish(p):
        q = VO.at[pl.ds(0, 5), 0, 0, 0, :, 0]
        got(q, xs.at[p])
        got(q, ys.at[p])
        @pl.when(mid)
        def _():
            got(q.at[:, pl.ds(0, 6)], zis.at[p])
            got(q, zos.at[p])
        @pl.when(jnp.logical_not(mid))
        def _(): got(q.at[:, pl.ds(0, 3)], zis.at[p])
        whole = VO.at[0, :, :, :, :, 0]
        got(whole, ds.at[p])
        got(whole, dr.at[p])
    over(NP, finish)


def place_kernel(VO, og, ou, od, sems):
    out = []
    def put(src, dst):
        out.append(copy(src, dst, sems.at[len(out)]))
        out[-1].start()
    parts = [(l, i) for l in range(L) for i in range(X)]
    for l, i in parts:
        put(VO.at[L + l, i], og.at[l, i])
        put(VO.at[2 * L + l, i], ou.at[l, i])
    for l, i in parts:
        for k in range(CORES): put(VO.at[l, i, :, :, :, k], od.at[l, i, :, :, k])
    for cp in out: cp.wait()


def ag_call(wgu, wd):
    four = DMA((NP, Z))
    one = DMA((NP,))
    VO = pl.pallas_call(
        functools.partial(ag_kernel, lagged(AG_ORDER)),
        out_shape=VMEM((NP, X, Y, Z, U, CORES, *T3), BF),
        in_specs=[HB] * 2,
        out_specs=VM,
        scratch_shapes=[VMEM((2, HALF, *T3), BF), DMA((NP + 1,)), DMA((HALF + 1,)), DMA((HALF + 1,))] + [one] * 6 + [DMA((NP, Z, 2)), four, four, four, four, one, four, one, one],
        compiler_params=pltpu.CompilerParams(collective_id=1, has_side_effects=True, vmem_limit_bytes=2**20),
        name="all_gather",
    )(pinned(wgu, HBM), pinned(wd, HBM))
    G = jax.ShapeDtypeStruct((L, X, Y, Z, U, CORES, *T3), BF)
    D = jax.ShapeDtypeStruct((L, X, Y, Z, CORES, U, *T3), BF)
    og, ou, od = pl.pallas_call(
        place_kernel, out_shape=(G, G, D), in_specs=[VM], out_specs=(ANY,) * 3, scratch_shapes=[DMA((16,))],
        compiler_params=pltpu.CompilerParams(vmem_limit_bytes=2**20), name="place",
    )(pinned(VO, VMEM))
    return og, ou, od


def solution(mesh):
    def step(*arrays):
        terms, weights, m, v = (arrays[i : i + 3] for i in range(0, 12, 3))
        moments = [f(a) for a, f in zip((*m, *v), (view_m, view_m, view_md) * 2)]
        *sums, _ = rs_call([t[0] for t in terms], weights, moments)
        Wgu, Wd, new = up_call(sums, weights, moments)
        whole = [untiled(a, *w.shape[1:]) for a, w in zip(ag_call(Wgu, Wd), weights)]
        return (*whole, *new)

    all_of, cut = P(None, None, None), P(None, "dp", None)
    return jax.shard_map(
        step,
        mesh=mesh,
        in_specs=(P(("rep", "dp"), None, None, None),) * 3 + (all_of,) * 3 + (cut,) * 6,
        out_specs=(P("rep", None, None),) * 3 + (P("rep", "dp", None),) * 6,
        check_vma=False,
    )
```
